32 devices in a mesh: replica: 1, ctx: 32 (over z, y, x, core).
Axes of the slice: x: 2, y: 2, z: 4, core: 2. Of those that a mesh axis runs over, the one named last changes fastest.
Arguments:
- queries: bfloat16 [128, 4096], P(('replica', 'ctx')), may hold values from -4 to 6.2
- own_key: bfloat16 [128, 256], P(('replica', 'ctx')), may hold values from -12 to 12
- own_value: bfloat16 [128, 256], P(('replica', 'ctx')), may hold values from -40 to 40
- cache_keys: bfloat16 [2, 1024, 256], P('replica', 'ctx'), may hold values from -4 to 4.7
- cache_values: bfloat16 [2, 1024, 256], P('replica', 'ctx'), may hold values from -40 to 40
- prefix_of_row: int32 [128], P('replica'), may hold values from 0 to 1, as said below
- context_len: int32 [2], P('replica'), may hold values from 512 to 1024
- hidden_in: bfloat16 [128, 4096], P(('replica', 'ctx')), may hold values from -3 to 3
- w_out: bfloat16 [4096, 4096], P('ctx'), may hold values from -0.09375 to 0.09375
- norm_gain: float32 [4096], replicated, may hold values from 0.5 to 1.5
- expert_ids: int32 [128, 8], P(('replica', 'ctx')), may hold values from 0 to 15, all different within a row; in each aligned block of 4 rows (0 to 3, 4 to 7, ...) at most 4 rows name the same one
- route_weights: float32 [128, 8], P(('replica', 'ctx')), may hold values from 0.05 to 0.4
- gate_up_codes: bfloat16 [32, 4096, 768], P('ctx'), may hold values from -0.09375 to 0.09375
- gate_up_scales: float32 [32, 32, 6], P('ctx'), may hold values from 0.6 to 1.7
- down_codes: bfloat16 [32, 384, 4096], P('ctx'), may hold values from -0.21875 to 0.21875
- down_scales: float32 [32, 3, 32], P('ctx'), may hold values from 0.6 to 1.7
Outputs:
- attention_out: bfloat16 [128, 4096], P(('replica', 'ctx'))
- layer_out: bfloat16 [128, 4096], P(('replica', 'ctx'))
The draws below stay inside these ranges and needn't reach their ends.
Inputs may be any that keep to these rules, and one draw needn't show every extreme that they name: `prefix_of_row`: the rows come in aligned blocks of 64 consecutive rows that all name one prefix. `expert_ids`: each row names 8 different experts; among the 4 rows of one device no expert is named more than 4 times.
All inputs are finite; a program needn't handle non-finite values.
Results may differ from the reference program's by a relative error of at most 0.014.
Values may be sent and summed in bfloat16 or wider, within the bound.
No kernel may reach another device: no remote copies, remote signals or barrier semaphores. Data moves between devices by JAX's collectives and lax.ppermute only.
A program may use at most 128 MiB of HBM per device.

```python
import math
import jax
import jax.numpy as jnp
import numpy as np
from jax import lax

D = 4096
QH = 32
KVH = 2
HD = 128
CTX_DEV = 32
CAND = 64
ROW_DEV = 4
TOP = 8
EXP_HID = 768
BLK = 128
DQ = 4096
DKV = 256
CTX = 1024
ROWS = 128
PREFIXES = 2
EXPERTS = 16
CAP = 4
N_CTX = 32


def draw_queries(key, part):
    key_base = jax.random.fold_in(jax.random.fold_in(key, 11), 0)
    drawn = jnp.clip(jax.random.normal(key_base, (ROWS, QH * HD), jnp.float32), -4.0, 4.0)
    return drawn.astype(jnp.bfloat16)


def draw_cache_keys(key, part):
    key_base = jax.random.fold_in(jax.random.fold_in(key, 23), 0)
    drawn = jnp.clip(jax.random.normal(key_base, (PREFIXES, CTX, KVH * HD), jnp.float32), -4.0, 4.0)
    return drawn.astype(jnp.bfloat16)


def draw_prefix_of_row(key, part):
    block_choice = jax.random.randint(jax.random.fold_in(key, 37), (PREFIXES,), 0, PREFIXES).astype(jnp.int32)
    block_of_row = (jnp.arange(ROWS, dtype=jnp.int32) // CAND).astype(jnp.int32)
    return jnp.take(block_choice, block_of_row).astype(jnp.int32)


def levels(stream_key, shape, cuts, smallest, top_value):
    loudness = 1.0
    for dim, blocks in cuts:
        draws = jax.random.uniform(jax.random.fold_in(jax.random.fold_in(stream_key, 6), dim), (blocks,), jnp.float32, smallest / len(cuts), top_value / len(cuts))
        loudness = loudness * jnp.repeat(jnp.exp(draws), shape[dim] // blocks).reshape((-1,) + (1,) * (len(shape) - 1 - dim))
    return loudness


def assign_block(stream_key, own, number, rows, number_of, top, limit, slope):
    order = jax.random.permutation(stream_key, number_of)
    heavy_load, usual = shares(number_of, rows * top, limit, slope, True), shares(number_of, rows * top, limit, slope, False)
    places = jnp.arange(number_of)

    def named(sizes, turn):
        used = int((sizes > 0).sum())
        fixed = max(1, used // 4)
        passed = fixed + (places - fixed + turn * (used - fixed)) % max(1, number_of - fixed)
        return jnp.zeros((number_of,), jnp.int32).at[order[jnp.where(places < fixed, places, passed)]].set(jnp.asarray(sizes, jnp.int32))

    sizes = jnp.where(number % 4 == 0, named(heavy_load, number // 4), named(usual, number - number // 4 - 1))
    mixed = jax.random.permutation(jax.random.fold_in(own, 3), number_of)
    source_of, receiver = mixed[0:number_of // 2 * 2:2], mixed[1:number_of // 2 * 2:2]
    slack = jnp.minimum(sizes[source_of] - 1, limit - sizes[receiver]) // 2
    slack = jnp.where((source_of == order[0]) | (receiver == order[0]) | (sizes[receiver] == 0), 0, jnp.maximum(slack, 0))
    passed = jax.random.randint(jax.random.fold_in(own, 4), (number_of // 2,), 0, 1 << 20) % (slack + 1)
    sizes = sizes.at[source_of].add(-passed).at[receiver].add(passed)
    labels = jnp.searchsorted(jnp.cumsum(sizes), jnp.arange(rows * top), side="right").astype(jnp.int32)
    grid = labels.reshape(top, rows).T
    grid = grid[jax.random.permutation(jax.random.fold_in(own, 1), rows)]
    turn = jax.random.randint(jax.random.fold_in(own, 2), (rows, 1), 0, top)
    return jnp.take_along_axis(grid, (jnp.arange(top)[None, :] + turn) % top, axis=1)


def shares(number_of, total, limit, skew, full):
    loads = [(1 << 20) // math.isqrt(rank ** skew) + 1 for rank in range(1, number_of + 1)]
    largest = limit if full else min(limit, max(-(-total // number_of), total * loads[0] // sum(loads)))
    least = 1 if total - largest >= number_of - 1 else 0
    given, surplus = [largest] + [least] * (number_of - 1), total - largest - least * (number_of - 1)
    while surplus > 0:
        candidates = [i for i in range(1, number_of) if given[i] < largest] or [i for i in range(1, number_of) if given[i] < limit]
        whole, budget = sum([loads[i] for i in candidates]), surplus
        for i in candidates:
            more = min(limit - given[i], max(1, budget * loads[i] // whole), surplus)
            given[i] = given[i] + more
            surplus = surplus - more
    return np.array(given)


def bell_draw(key, dims, width, bound, cuts=(), kind=jnp.bfloat16):
    array = jax.random.normal(key, dims, jnp.float32) * width
    if len(cuts) > 0:
        array = levels(key, dims, cuts, -0.22, 0.18) * array
    return jnp.clip(array, min=-bound, max=bound).astype(kind)


def setup_inputs(seed: int = 0, part: int = 0) -> dict:
    key_of = jax.random.split(jax.random.key(seed), 17)
    part_splits = jax.random.split(jax.random.fold_in(key_of[16], part), 17)
    queries = draw_queries(jax.random.fold_in(jax.random.fold_in(key_of[16], part), 71), part)
    own_key = bell_draw(part_splits[1], (ROWS, DKV), 3.0, 12.0, ((0, 32),))
    own_value = bell_draw(part_splits[2], (ROWS, DKV), 8.0, 40.0, ((0, 32),))
    cache_keys = draw_cache_keys(jax.random.fold_in(jax.random.fold_in(key_of[16], part), 71), part)
    cache_values = bell_draw(part_splits[4], (PREFIXES, CTX, DKV), 8.0, 40.0, ((1, 32),))
    prefix_of_row = draw_prefix_of_row(jax.random.fold_in(jax.random.fold_in(key_of[16], part), 71), part)
    context_len = jax.random.randint(part_splits[6], (PREFIXES,), CTX // 2, CTX + 1).astype(jnp.int32)
    hidden_in = bell_draw(part_splits[7], (ROWS, D), 0.5, 3.0, ((0, 32),))
    w_out = bell_draw(key_of[8], (DQ, D), DQ ** -0.5, 0.09375, ((0, 32),))
    norm_gain = jnp.clip(1.0 + 0.1 * jax.random.normal(key_of[9], (D,), jnp.float32), 0.5, 1.5)
    expert_ids_keys = jax.random.split(jax.random.fold_in(part_splits[10], 1), ROWS // ROW_DEV)
    expert_ids_turns = jax.random.permutation(jax.random.fold_in(part_splits[10], 3), ROWS // ROW_DEV)
    expert_ids = jax.vmap(lambda own, number: assign_block(jax.random.fold_in(part_splits[10], 2), own, number, ROW_DEV, EXPERTS, TOP, CAP, 2))(expert_ids_keys, expert_ids_turns).reshape((ROWS, TOP))
    route_weights = jnp.clip(jnp.exp(math.log(0.4) - 2.0794415 * jax.random.uniform(part_splits[11], (ROWS, TOP), jnp.float32) ** levels(part_splits[11], (ROWS, TOP), ((0, 32),), -0.2, 0.2)), 0.05, 0.4)
    gate_up_codes = bell_draw(key_of[12], (2 * EXPERTS, D, EXP_HID), D ** -0.5, 0.09375, ((0, 32),))
    gate_up_scales = jnp.clip(jnp.exp(math.log(1.7) - 1.04145386 * jax.random.uniform(key_of[13], (2 * EXPERTS, D // BLK, EXP_HID // BLK), jnp.float32) ** levels(key_of[13], (2 * EXPERTS, D // BLK, EXP_HID // BLK), ((0, 32),), -0.2, 0.2)), 0.6, 1.7)
    down_codes = bell_draw(key_of[14], (2 * EXPERTS, EXP_HID // 2, D), EXP_HID ** -0.5, 0.21875, ((0, 32),))
    down_scales = jnp.clip(jnp.exp(math.log(1.7) - 1.04145386 * jax.random.uniform(key_of[15], (2 * EXPERTS, EXP_HID // (2 * BLK), D // BLK), jnp.float32) ** levels(key_of[15], (2 * EXPERTS, EXP_HID // (2 * BLK), D // BLK), ((0, 32),), -0.2, 0.2)), 0.6, 1.7)
    return dict(queries=queries, own_key=own_key, own_value=own_value, cache_keys=cache_keys, cache_values=cache_values, prefix_of_row=prefix_of_row, context_len=context_len, hidden_in=hidden_in, w_out=w_out, norm_gain=norm_gain, expert_ids=expert_ids, route_weights=route_weights, gate_up_codes=gate_up_codes, gate_up_scales=gate_up_scales, down_codes=down_codes, down_scales=down_scales)


NEG = -1e+30
EPSILON = 1e-06

def dequantize(code_values, scales):
    rows_per = code_values.shape[0] // scales.shape[0]
    cols_per = code_values.shape[1] // scales.shape[1]
    spread = jnp.repeat(jnp.repeat(scales, rows_per, axis=0), cols_per, axis=1)
    return (code_values.astype(jnp.float32) * spread).astype(jnp.bfloat16)

def reference(queries, own_key, own_value, cache_keys, cache_values, prefix_of_row, context_len, hidden_in, w_out, norm_gain, expert_ids, route_weights, gate_up_codes, gate_up_scales, down_codes, down_scales):
    row_total = queries.shape[0]
    per_group = QH // KVH
    score_scale = 1.0 / math.sqrt(HD)
    position = jnp.arange(CTX, dtype=jnp.int32).reshape(N_CTX, CTX_DEV)

    def attend_row(row_index):
        prefix = prefix_of_row[row_index]
        length = context_len[prefix]
        key_block = cache_keys[prefix].astype(jnp.float32).reshape(N_CTX, CTX_DEV, KVH, HD)
        values = cache_values[prefix].astype(jnp.float32).reshape(N_CTX, CTX_DEV, KVH, HD)
        query_heads = queries[row_index].astype(jnp.float32).reshape(KVH, per_group, HD)
        scores = jnp.einsum('gqd,ctgd->cgqt', query_heads, key_block) * score_scale
        is_valid = (position < length)[:, None, None, :]
        masked = jnp.where(is_valid, scores, NEG)
        block_max = lax.optimization_barrier(jnp.max(masked, axis=-1))
        weights = jnp.where(is_valid, jnp.exp(masked - block_max[..., None]), 0.0)
        block_total = lax.optimization_barrier(jnp.sum(weights, axis=-1))
        rounded = lax.optimization_barrier(weights.astype(jnp.bfloat16)).astype(jnp.float32)
        numerator = jnp.einsum('cgqt,ctgd->cgqd', rounded, values)
        block_out = numerator / jnp.maximum(block_total, 1.0)[..., None]
        block_out = lax.optimization_barrier(block_out.astype(jnp.bfloat16)).astype(jnp.float32)
        own_keys = own_key[row_index].astype(jnp.float32).reshape(KVH, HD)
        own_score = jnp.einsum('gqd,gd->gq', query_heads, own_keys) * score_scale
        top_score = jnp.maximum(lax.optimization_barrier(jnp.max(block_max, axis=0)), own_score)
        factor = block_total * jnp.exp(block_max - top_score[None])
        own_weight = jnp.exp(own_score - top_score)
        own_values = own_value[row_index].astype(jnp.float32).reshape(KVH, 1, HD)
        numerator_all = lax.optimization_barrier(jnp.sum(factor[..., None] * block_out, axis=0)) + own_weight[..., None] * own_values
        denominator = lax.optimization_barrier(jnp.sum(factor, axis=0)) + own_weight
        return (numerator_all / denominator[..., None]).reshape(QH * HD).astype(jnp.bfloat16)
    attended = lax.map(attend_row, jnp.arange(row_total, dtype=jnp.int32))
    mixed = hidden_in.astype(jnp.float32) + jnp.dot(attended, w_out, preferred_element_type=jnp.float32)
    attention_out = mixed.astype(jnp.bfloat16)
    mean_square = lax.optimization_barrier(jnp.mean(mixed * mixed, axis=-1, keepdims=True))
    normed = (mixed * lax.rsqrt(mean_square + EPSILON) * norm_gain).astype(jnp.bfloat16)
    pick_ids = expert_ids.reshape(-1).astype(jnp.int32)
    pick_count = pick_ids.shape[0]
    pick_row = (jnp.arange(pick_count, dtype=jnp.int32) // TOP).astype(jnp.int32)
    pick_weight = route_weights.reshape(-1)
    sorted_picks = jnp.argsort(pick_ids, stable=True).astype(jnp.int32)
    counts = lax.optimization_barrier(jnp.sum((pick_ids[None, :] == jnp.arange(EXPERTS, dtype=jnp.int32)[:, None]).astype(jnp.int32), axis=1))
    starts = (jnp.cumsum(counts) - counts).astype(jnp.int32)
    window = N_CTX * CAP
    padded_order = jnp.concatenate([sorted_picks, jnp.zeros((window,), jnp.int32)])
    half_width = EXP_HID // 2

    def add_expert(expert, running):
        chosen = lax.dynamic_slice_in_dim(padded_order, starts[expert], window)
        is_live = jnp.arange(window, dtype=jnp.int32) < counts[expert]
        inputs = normed[pick_row[chosen]]
        result = jnp.zeros((window, D), jnp.float32)
        for part_half in range(2):
            entry = 2 * expert + part_half
            gate_up = dequantize(lax.dynamic_index_in_dim(gate_up_codes, entry, 0, False), lax.dynamic_index_in_dim(gate_up_scales, entry, 0, False))
            down_proj = dequantize(lax.dynamic_index_in_dim(down_codes, entry, 0, False), lax.dynamic_index_in_dim(down_scales, entry, 0, False))
            projected_in = jnp.dot(inputs, gate_up, preferred_element_type=jnp.float32)
            activated = (jax.nn.silu(projected_in[:, :half_width]) * projected_in[:, half_width:]).astype(jnp.bfloat16)
            piece_out = jnp.dot(activated, down_proj, preferred_element_type=jnp.float32)
            result = result + lax.optimization_barrier(piece_out.astype(jnp.bfloat16)).astype(jnp.float32)
        scaled = jnp.where(is_live, pick_weight[chosen], 0.0)[:, None] * result
        return running.at[pick_row[chosen]].add(scaled)
    expert_sum = lax.fori_loop(0, EXPERTS, add_expert, jnp.zeros((row_total, D), jnp.float32))
    layer_out = (mixed + expert_sum).astype(jnp.bfloat16)
    return (attention_out, layer_out)
```

```python
import functools
import math

import jax
import jax.numpy as jnp
from jax import lax
from jax.experimental import pallas as pl
from jax.experimental.pallas import tpu as pltpu
from jax.sharding import PartitionSpec as P

HD = 128
CAND = 64

NEG = -1e30
EPSILON = 1e-06
LOW = 2
MID = 4


def swapped(value, offset):
    return lax.ppermute(value, "ctx", [(i, i ^ offset) for i in range(lax.axis_size("ctx"))])


def stage_offsets(shards):
    low = [i for i in range(LOW)]
    mid = [i * LOW for i in range(MID)]
    high = [i * LOW * MID for i in range(shards // (LOW * MID))]
    return low, mid, high


def dequantize(code_values, scales):
    rows_per = code_values.shape[0] // scales.shape[0]
    cols_per = code_values.shape[1] // scales.shape[1]
    spread = jnp.repeat(jnp.repeat(scales, rows_per, axis=0), cols_per, axis=1)
    return (code_values.astype(jnp.float32) * spread).astype(jnp.bfloat16)


def pack_body(info, q, own_key, own_value, keys, values, *outs, feature, per_group):
    device = info[0]
    prefixes, ctx_local, _ = keys.shape
    rows = q.shape[0]
    kv_rows = prefixes * ctx_local

    def head_of(target):
        return (target * feature) // HD

    for zx, out in enumerate(outs):
        group = head_of(device ^ (zx * LOW * MID)) // per_group
        lanes = pl.ds(pl.multiple_of(group * HD, HD), HD)
        out[0:kv_rows, 0:HD] = keys[:, :, lanes].reshape(kv_rows, HD)
        out[0:kv_rows, HD : 2 * HD] = values[:, :, lanes].reshape(kv_rows, HD)
        for mx in range(MID):
            top = kv_rows + mx * rows
            for cx in range(LOW):
                head = head_of(device ^ (zx * LOW * MID + mx * LOW + cx))
                out[top : top + rows, cx * HD : (cx + 1) * HD] = q[:, pl.ds(pl.multiple_of(head * HD, HD), HD)]
        top = kv_rows + MID * rows
        out[top : top + rows, 0:HD] = own_key[:, lanes]
        out[top : top + rows, HD : 2 * HD] = own_value[:, lanes]


def repack_body(*refs, kv_rows, rows):
    outs = refs[-MID:]
    parts = refs[:-MID]
    for zx, part in enumerate(parts):
        for mx, out in enumerate(outs):
            out[zx, 0:kv_rows, :] = part[0:kv_rows, :]
            top = kv_rows + mx * rows
            own = kv_rows + MID * rows
            out[zx, kv_rows : kv_rows + rows, :] = part[top : top + rows, :]
            out[zx, kv_rows + rows : kv_rows + 2 * rows, :] = part[own : own + rows, :]


def attend_body(info, prefix_of, lengths, mine, other, w_out, keep, send, att, *, ctx_local, kv_rows, rows):
    device = info[0]
    mid, high = mine.shape[0], mine.shape[1]
    pieces = mid * high
    span = CAND // (LOW * mid * rows)
    scale = 1.0 / math.sqrt(HD)
    tile = 2 * rows
    pick_rows = lax.broadcasted_iota(jnp.int32, (CAND, CAND * 2), 0)
    pick_cols = lax.broadcasted_iota(jnp.int32, (CAND, CAND * 2), 1)
    wanted = pick_rows // rows * tile + pick_rows % rows
    pick_query = (pick_cols == wanted).astype(jnp.bfloat16)
    pick_own = (pick_cols == wanted + rows).astype(jnp.bfloat16)
    column = lax.broadcasted_iota(jnp.int32, (CAND, pieces * ctx_local), 1)
    piece = column // ctx_local
    within = column % ctx_local
    relative = (piece % high) * (LOW * MID) + (piece // high) * LOW
    own_group = device // (LOW * mid * span)
    for zg in range(high // span):
        prefix = prefix_of[own_group ^ zg]
        length = lengths[prefix]
        zs = slice(zg * span, (zg + 1) * span)
        tail_mine = mine[:, zs, kv_rows : kv_rows + tile, :].reshape(CAND, 2 * HD)
        tail_other = other[:, zs, kv_rows : kv_rows + tile, :].reshape(CAND, 2 * HD)
        padded = jnp.concatenate([tail_mine[:, 0:HD], tail_other[:, HD : 2 * HD]], axis=0)
        query = jnp.dot(pick_query, padded, preferred_element_type=jnp.float32)
        own = jnp.dot(
            pick_own, jnp.concatenate([tail_mine, tail_other], axis=0), preferred_element_type=jnp.float32
        )
        own_score = jnp.sum(query * own[:, 0:HD], axis=1, keepdims=True) * scale
        query = query.astype(jnp.bfloat16)
        top = own_score
        all_scores = []
        for cx, source in enumerate((mine, other)):
            at = pl.ds(pl.multiple_of(prefix * ctx_local, ctx_local), ctx_local)
            key = source[:, :, at, 0:HD].reshape(pieces * ctx_local, HD)
            scores = (
                lax.dot_general(query, key, (((1,), (1,)), ((), ())), preferred_element_type=jnp.float32) * scale
            )
            position = (device ^ (relative + cx)) * ctx_local + within
            scores = jnp.where(position < length, scores, NEG)
            top = jnp.maximum(top, jnp.max(scores, axis=1, keepdims=True))
            all_scores.append(scores)
        own_weight = jnp.exp(own_score - top)
        numer = own_weight * own[:, HD : 2 * HD]
        denom = own_weight
        for scores, source in zip(all_scores, (mine, other)):
            at = pl.ds(pl.multiple_of(prefix * ctx_local, ctx_local), ctx_local)
            value = source[:, :, at, HD : 2 * HD].reshape(pieces * ctx_local, HD)
            weights = jnp.exp(scores - top)
            denom = denom + jnp.sum(weights, axis=1, keepdims=True)
            numer = numer + jnp.dot(weights.astype(jnp.bfloat16), value, preferred_element_type=jnp.float32)
        attended = numer / denom
        chunk = span * rows
        att[:, zg * chunk : (zg + 1) * chunk, :] = attended.reshape(LOW * mid, chunk, HD)
    half = keep.shape[0]
    attended = att[...].reshape(2 * half, HD).astype(jnp.bfloat16)
    keep[...] = jnp.dot(attended[0:half], w_out[...], preferred_element_type=jnp.float32)
    send[...] = jnp.dot(attended[half:], w_out[...], preferred_element_type=jnp.float32).astype(jnp.bfloat16)


VMEM = pl.BlockSpec(memory_space=pltpu.VMEM)
SMEM = pl.BlockSpec(memory_space=pltpu.SMEM)


def scatter_sum(keep, send, mid, high):
    width = keep.shape[1]
    summed = keep + swapped(send, 1).astype(jnp.float32)
    for offsets in (mid, high):
        parts = summed.reshape(len(offsets), -1, width)
        total = parts[0]
        got = [swapped(parts[i].astype(jnp.bfloat16), offsets[i]) for i in range(1, len(offsets))]
        for item in got:
            total = total + item.astype(jnp.float32)
        summed = total
    return summed


def local(
    queries,
    own_key,
    own_value,
    cache_keys,
    cache_values,
    prefix_of_row,
    context_len,
    hidden_in,
    w_out,
    norm_gain,
    expert_ids,
    route_weights,
    gate_up_codes,
    gate_up_scales,
    down_codes,
    down_scales,
):
    shards = lax.axis_size("ctx")
    device = lax.axis_index("ctx")
    rows = queries.shape[0]
    width = hidden_in.shape[1]
    key_groups = own_key.shape[1] // HD
    head_count = queries.shape[1] // HD
    per_group = head_count // key_groups
    prefixes, ctx_local, _ = cache_keys.shape
    kv_rows = prefixes * ctx_local
    feature = w_out.shape[0]
    low, mid, high = stage_offsets(shards)
    info = device.reshape(1).astype(jnp.int32)
    block_prefix = prefix_of_row.reshape(-1, CAND)[:, 0]

    message_rows = kv_rows + MID * rows + 2 * rows
    messages = pl.pallas_call(
        functools.partial(pack_body, feature=feature, per_group=per_group),
        in_specs=[SMEM] + [VMEM] * 5,
        out_specs=[VMEM] * len(high),
        out_shape=[jax.ShapeDtypeStruct((message_rows, 2 * HD), jnp.bfloat16)] * len(high),
        name="pack",
    )(info, queries, own_key, own_value, cache_keys, cache_values)
    got = [messages[0]] + [swapped(messages[i], high[i]) for i in range(1, len(high))]
    piece = jax.ShapeDtypeStruct((len(high), kv_rows + 2 * rows, 2 * HD), jnp.bfloat16)
    messages = pl.pallas_call(
        functools.partial(repack_body, kv_rows=kv_rows, rows=rows),
        in_specs=[VMEM] * len(high),
        out_specs=[VMEM] * MID,
        out_shape=[piece] * MID,
        name="repack",
    )(*got)
    mine = jnp.stack([messages[0]] + [swapped(messages[i], mid[i]) for i in range(1, MID)], axis=0)
    other = swapped(mine, low[1])

    if feature < HD:
        w_full = lax.dynamic_update_slice(
            jnp.zeros((HD, w_out.shape[1]), w_out.dtype), w_out, ((device * feature) % HD, 0)
        )
    else:
        w_full = w_out
    half = shards * rows // 2
    keep, send = pl.pallas_call(
        functools.partial(attend_body, ctx_local=ctx_local, kv_rows=kv_rows, rows=rows),
        in_specs=[SMEM] * 3 + [VMEM] * 3,
        out_specs=[VMEM] * 2,
        out_shape=[
            jax.ShapeDtypeStruct((half, width), jnp.float32),
            jax.ShapeDtypeStruct((half, width), jnp.bfloat16),
        ],
        scratch_shapes=[pltpu.VMEM((LOW * MID, len(high) * rows, HD), jnp.float32)],
        name="attend",
    )(info, block_prefix, context_len, mine, other, w_full)

    projected = scatter_sum(keep, send, mid, high)
    mixed = hidden_in.astype(jnp.float32) + projected
    attention_out = mixed.astype(jnp.bfloat16)
    mean_square = jnp.mean(mixed * mixed, axis=-1, keepdims=True)
    normed = (mixed * lax.rsqrt(mean_square + EPSILON) * norm_gain).astype(jnp.bfloat16)

    experts_all = shards // 2
    hit = expert_ids[:, :, None] == jnp.arange(experts_all, dtype=jnp.int32)[None, None, :]
    combine = jnp.sum(jnp.where(hit, route_weights[:, :, None], 0.0), axis=1)
    coarse = lax.reduce_precision(combine, 8, 7)
    fine = combine - coarse
    extra = -(2 * experts_all) % HD
    tail = jnp.concatenate([coarse, fine, jnp.zeros((rows, extra), jnp.float32)], axis=1)
    held = jnp.concatenate([normed, tail.astype(jnp.bfloat16)], axis=1)
    for offsets in (high, mid, low):
        held = jnp.concatenate([held] + [swapped(held, o) for o in offsets[1:]], axis=0)
    lane = lax.broadcasted_iota(jnp.int32, (1, 2 * experts_all + extra), 1)
    expert = device // 2
    chosen = (lane == expert) | (lane == expert + experts_all)
    row_weight = jnp.sum(jnp.where(chosen, held[:, width:].astype(jnp.float32), 0.0), axis=1, keepdims=True)

    gate_up = dequantize(gate_up_codes[0], gate_up_scales[0])
    down_proj = dequantize(down_codes[0], down_scales[0])
    half_width = down_proj.shape[0]
    projected_in = jnp.dot(held[:, :width], gate_up, preferred_element_type=jnp.float32)
    activated = (jax.nn.silu(projected_in[:, :half_width]) * projected_in[:, half_width:]).astype(jnp.bfloat16)
    result = jnp.dot(activated, down_proj, preferred_element_type=jnp.float32) * row_weight
    expert_sum = scatter_sum(result[:half], result[half:].astype(jnp.bfloat16), mid, high)
    layer_out = (mixed + expert_sum).astype(jnp.bfloat16)
    return (attention_out, layer_out)


def solution(mesh):
    return jax.shard_map(
        local,
        mesh=mesh,
        in_specs=(
            P(("replica", "ctx"), None),
            P(("replica", "ctx"), None),
            P(("replica", "ctx"), None),
            P("replica", "ctx", None),
            P("replica", "ctx", None),
            P("replica"),
            P("replica"),
            P(("replica", "ctx"), None),
            P("ctx", None),
            P(),
            P(("replica", "ctx"), None),
            P(("replica", "ctx"), None),
            P("ctx", None, None),
            P("ctx", None, None),
            P("ctx", None, None),
            P("ctx", None, None),
        ),
        out_specs=(P(("replica", "ctx"), None), P(("replica", "ctx"), None)),
        check_vma=False,
    )
```

```python
import functools
import math

import jax
import jax.numpy as jnp
from jax import lax
from jax.experimental import pallas as pl
from jax.experimental.pallas import tpu as pltpu
from jax.sharding import PartitionSpec as P


HD = 128
CAND = 64

NEG = -1e30
EPSILON = 1e-06
LOW = 2
MID = 4
BLK = 128
STRIP = 2**19
DEPTH = 4
SMALL_VMEM = 8 * 2**20


def swapped(value, offset):
    return lax.ppermute(value, "ctx", [(i, i ^ offset) for i in range(lax.axis_size("ctx"))])


def in_hbm(value):
    return pltpu.with_memory_space_constraint(value, pltpu.HBM)


def stage_offsets(shards):
    low = [i for i in range(LOW)]
    mid = [i * LOW for i in range(MID)]
    high = [i * LOW * MID for i in range(shards // (LOW * MID))]
    return low, mid, high


def pack_body(*refs, feature, per_group, count):
    sources, outs, held, sems = refs[:5], refs[5 : 5 + count], refs[5 + count : 10 + count], refs[10 + count]
    copies = [pltpu.make_async_copy(source, to, sems.at[i]) for i, (source, to) in enumerate(zip(sources, held))]
    for copy in copies:
        copy.start()
    for copy in copies:
        copy.wait()
    q, own_key, own_value, keys, values = held
    device = lax.axis_index("ctx")
    prefixes, ctx_local, _ = keys.shape
    rows = q.shape[0]
    kv_rows = prefixes * ctx_local

    def head_of(target):
        return (target * feature) // HD

    for zx, out in enumerate(outs):
        group = head_of(device ^ (zx * LOW * MID)) // per_group
        lanes = pl.ds(pl.multiple_of(group * HD, HD), HD)
        out[0:kv_rows, 0:HD] = keys[:, :, lanes].reshape(kv_rows, HD)
        out[0:kv_rows, HD : 2 * HD] = values[:, :, lanes].reshape(kv_rows, HD)
        for mx in range(MID):
            top = kv_rows + mx * rows
            for cx in range(LOW):
                head = head_of(device ^ (zx * LOW * MID + mx * LOW + cx))
                out[top : top + rows, cx * HD : (cx + 1) * HD] = q[:, pl.ds(pl.multiple_of(head * HD, HD), HD)]
        top = kv_rows + MID * rows
        out[top : top + rows, 0:HD] = own_key[:, lanes]
        out[top : top + rows, HD : 2 * HD] = own_value[:, lanes]


def repack_body(after, *refs, kv_rows, rows):
    outs = refs[-MID:]
    parts = refs[:-MID]
    for zx, part in enumerate(parts):
        for mx, out in enumerate(outs):
            out[zx, 0:kv_rows, :] = part[0:kv_rows, :]
            top = kv_rows + mx * rows
            own = kv_rows + MID * rows
            out[zx, kv_rows : kv_rows + rows, :] = part[top : top + rows, :]
            out[zx, kv_rows + rows : kv_rows + 2 * rows, :] = part[own : own + rows, :]


def attend_body(info, *refs, ctx_local, kv_rows, rows):
    mine, other = refs[:MID], refs[MID : 2 * MID]
    w_out, keep, send, att = refs[2 * MID :]
    device = lax.axis_index("ctx")
    high = mine[0].shape[0]
    pieces = MID * high
    span = CAND // (LOW * MID * rows)
    scale = 1.0 / math.sqrt(HD)
    tile = 2 * rows
    pick_rows = lax.broadcasted_iota(jnp.int32, (CAND, CAND * 2), 0)
    pick_cols = lax.broadcasted_iota(jnp.int32, (CAND, CAND * 2), 1)
    wanted = pick_rows // rows * tile + pick_rows % rows
    pick_query = (pick_cols == wanted).astype(jnp.bfloat16)
    pick_own = (pick_cols == wanted + rows).astype(jnp.bfloat16)
    column = lax.broadcasted_iota(jnp.int32, (CAND, pieces * ctx_local), 1)
    piece = column // ctx_local
    within = column % ctx_local
    relative = (piece % high) * (LOW * MID) + (piece // high) * LOW
    own_group = device // (LOW * MID * span)

    def joined(parts, zs, at, lanes, depth):
        return jnp.concatenate([part[zs, at, lanes].reshape(depth, -1) for part in parts], axis=0)

    for zg in range(high // span):
        prefix = info[own_group ^ zg]
        length = info[high // span + prefix]
        zs = slice(zg * span, (zg + 1) * span)
        tails = slice(kv_rows, kv_rows + tile)
        at = pl.ds(pl.multiple_of(prefix * ctx_local, ctx_local), ctx_local)
        every = slice(0, high)
        tail_mine = joined(mine, zs, tails, slice(0, 2 * HD), span * tile)
        tail_other = joined(other, zs, tails, slice(0, 2 * HD), span * tile)
        padded = jnp.concatenate([tail_mine[:, 0:HD], tail_other[:, HD : 2 * HD]], axis=0)
        query = jnp.dot(pick_query, padded, preferred_element_type=jnp.float32)
        own = jnp.dot(
            pick_own, jnp.concatenate([tail_mine, tail_other], axis=0), preferred_element_type=jnp.float32
        )
        own_score = jnp.sum(query * own[:, 0:HD], axis=1, keepdims=True) * scale
        query = query.astype(jnp.bfloat16)
        top = own_score
        all_scores = []
        for cx, source in enumerate((mine, other)):
            key = joined(source, every, at, slice(0, HD), high * ctx_local)
            scores = (
                lax.dot_general(query, key, (((1,), (1,)), ((), ())), preferred_element_type=jnp.float32) * scale
            )
            position = (device ^ (relative + cx)) * ctx_local + within
            scores = jnp.where(position < length, scores, NEG)
            top = jnp.maximum(top, jnp.max(scores, axis=1, keepdims=True))
            all_scores.append(scores)
        own_weight = jnp.exp(own_score - top)
        numer = own_weight * own[:, HD : 2 * HD]
        denom = own_weight
        for scores, source in zip(all_scores, (mine, other)):
            value = joined(source, every, at, slice(HD, 2 * HD), high * ctx_local)
            weights = jnp.exp(scores - top)
            denom = denom + jnp.sum(weights, axis=1, keepdims=True)
            numer = numer + jnp.dot(weights.astype(jnp.bfloat16), value, preferred_element_type=jnp.float32)
        attended = numer / denom
        chunk = span * rows
        att[:, zg * chunk : (zg + 1) * chunk, :] = attended.reshape(LOW * MID, chunk, HD)
    half = keep.shape[0]
    attended = att[...].reshape(2 * half, HD).astype(jnp.bfloat16)
    out = jnp.dot(attended, w_out[...], preferred_element_type=jnp.float32)
    keep[...] = out[0:half]
    send[...] = out[half:].astype(jnp.bfloat16)


def dequantize_strips(out, codes, scales, first, count, offset):
    for i in range(first, first + count):
        rows = slice(i * BLK, (i + 1) * BLK)
        for j in range(codes.shape[1] // BLK):
            lanes = slice(j * BLK, (j + 1) * BLK)
            out[rows, lanes] = (codes[rows, lanes].astype(jnp.float32) * scales[offset + i, j]).astype(jnp.bfloat16)


def strip_rows(shape):
    blocks = shape[0] // BLK
    count = max(1, min(blocks, STRIP // (BLK * shape[1])))
    while blocks % count:
        count -= 1
    return count * BLK


def prepare_body(*refs, ranges, fetched):
    count = len(ranges)
    scales, sources, plain = refs[:count], refs[count : 2 * count], refs[2 * count : 2 * count + fetched]
    refs = refs[2 * count + fetched :]
    outs, fetch, held, sems = refs[:count], refs[count : count + fetched], refs[count + fetched : -1], refs[-1]
    jobs = []
    for scale, source, to, out, (start, size) in zip(scales, sources, held, outs, ranges):
        step = strip_rows((size, source.shape[1]))
        for first in range(0, size, step):
            copy = pltpu.make_async_copy(
                source.at[pl.ds(start + first, step)], to.at[pl.ds(first, step)], sems.at[len(jobs)]
            )
            jobs.append((copy, (out, to, scale, first // BLK, step // BLK, start // BLK)))
    direct = [pltpu.make_async_copy(a, to, sems.at[len(jobs) + i]) for i, (a, to) in enumerate(zip(plain, fetch))]
    for copy, _ in jobs[:DEPTH]:
        copy.start()
    for copy in direct:
        copy.start()
    for i, (copy, job) in enumerate(jobs):
        copy.wait()
        if i + DEPTH < len(jobs):
            jobs[i + DEPTH][0].start()
        dequantize_strips(*job)
    for copy in direct:
        copy.wait()


def prepared(weights, fetch=()):
    scales = [item[0] for item in weights]
    codes = [item[1] for item in weights]
    ranges = tuple(item[2:] for item in weights)
    fetch = list(fetch)
    shapes = [(size, a.shape[1]) for a, (_, size) in zip(codes, ranges)]
    steps = sum(shape[0] // strip_rows(shape) for shape in shapes)
    return pl.pallas_call(
        functools.partial(prepare_body, ranges=ranges, fetched=len(fetch)),
        in_specs=[SMEM] * len(codes) + [HBM] * (len(codes) + len(fetch)),
        out_specs=[VMEM] * (len(codes) + len(fetch)),
        out_shape=[pltpu.VMEM(shape, jnp.bfloat16) for shape in shapes] + [pltpu.VMEM(a.shape, a.dtype) for a in fetch],
        scratch_shapes=[pltpu.VMEM(shape, jnp.bfloat16) for shape in shapes]
        + [pltpu.SemaphoreType.DMA((steps + len(fetch),))],
        compiler_params=pltpu.CompilerParams(vmem_limit_bytes=2 * sum(math.prod(shape) for shape in shapes) + 2**20),
        name="prepare",
    )(*scales, *(in_hbm(item) for item in codes + fetch))


def join_body(*refs):
    out = refs[-1]
    rows = refs[0].shape[0]
    for i, part in enumerate(refs[:-1]):
        out[i * rows : (i + 1) * rows, :] = part[...]


def joined(parts):
    rows, width = parts[0].shape
    return pl.pallas_call(
        join_body,
        in_specs=[VMEM] * len(parts),
        out_specs=VMEM,
        out_shape=jax.ShapeDtypeStruct((len(parts) * rows, width), parts[0].dtype),
        compiler_params=pltpu.CompilerParams(vmem_limit_bytes=SMALL_VMEM),
        name="join",
    )(*parts)


def expert_body(*refs, width, experts):
    parts = refs[: 2 * MID]
    gate_first, gate_rest, down, keep, send, x = refs[2 * MID :]
    expert = lax.axis_index("ctx") // 2
    some = parts[0].shape[0]
    half = keep.shape[0]
    for i, part in enumerate(parts):
        x[i * some : (i + 1) * some, :] = part[:, 0:width]
    tail = jnp.concatenate([part[:, width:] for part in parts], axis=0).astype(jnp.float32)
    lane = lax.broadcasted_iota(jnp.int32, tail.shape, 1)
    chosen = (lane == expert) | (lane == expert + experts)
    weight = jnp.sum(jnp.where(chosen, tail, 0.0), axis=1, keepdims=True)
    hidden = down.shape[0]
    first = gate_first.shape[0]
    act = jnp.dot(x[:, :first], gate_first[...], preferred_element_type=jnp.float32)
    act += jnp.dot(x[:, first:], gate_rest[...], preferred_element_type=jnp.float32)
    gate, up = act[:, :hidden], act[:, hidden:]
    active = (gate / (1.0 + jnp.exp(-gate)) * up).astype(jnp.bfloat16)
    out = jnp.dot(active, down[...], preferred_element_type=jnp.float32) * weight
    keep[...] = out[0:half]
    send[...] = out[half:].astype(jnp.bfloat16)


VMEM = pl.BlockSpec(memory_space=pltpu.VMEM)
SMEM = pl.BlockSpec(memory_space=pltpu.SMEM)
HBM = pl.BlockSpec(memory_space=pltpu.HBM)
ANY = pl.BlockSpec(memory_space=pl.ANY)


def scatter_sum(keep, send, mid, high):
    width = keep.shape[1]
    summed = keep + swapped(send, 1).astype(jnp.float32)
    for offsets in (mid, high):
        parts = summed.reshape(len(offsets), -1, width)
        total = parts[0]
        got = [swapped(parts[i].astype(jnp.bfloat16), offsets[i]) for i in range(1, len(offsets))]
        for item in got:
            total = total + item.astype(jnp.float32)
        summed = total
    return summed


def local(
    queries,
    own_key,
    own_value,
    cache_keys,
    cache_values,
    prefix_of_row,
    context_len,
    hidden_in,
    w_out,
    norm_gain,
    expert_ids,
    route_weights,
    gate_up_codes,
    gate_up_scales,
    down_codes,
    down_scales,
):
    shards = lax.axis_size("ctx")
    device = lax.axis_index("ctx")
    rows = queries.shape[0]
    width = hidden_in.shape[1]
    key_groups = own_key.shape[1] // HD
    head_count = queries.shape[1] // HD
    per_group = head_count // key_groups
    prefixes, ctx_local, _ = cache_keys.shape
    kv_rows = prefixes * ctx_local
    feature = w_out.shape[0]
    low, mid, high = stage_offsets(shards)
    info = jnp.concatenate([prefix_of_row[::CAND], context_len])

    inputs = (queries, own_key, own_value, cache_keys, cache_values)
    message = jax.ShapeDtypeStruct((kv_rows + MID * rows + 2 * rows, 2 * HD), jnp.bfloat16)
    messages = pl.pallas_call(
        functools.partial(pack_body, feature=feature, per_group=per_group, count=len(high)),
        in_specs=[HBM] * len(inputs),
        out_specs=[VMEM] * len(high),
        out_shape=[message] * len(high),
        scratch_shapes=[pltpu.VMEM(a.shape, a.dtype) for a in inputs] + [pltpu.SemaphoreType.DMA((len(inputs),))],
        compiler_params=pltpu.CompilerParams(vmem_limit_bytes=SMALL_VMEM),
        name="pack",
    )(*(in_hbm(item) for item in inputs))
    got = [messages[0]] + [swapped(messages[i], high[i]) for i in range(1, len(high))]
    piece = jax.ShapeDtypeStruct((len(high), kv_rows + 2 * rows, 2 * HD), jnp.bfloat16)
    messages = pl.pallas_call(
        functools.partial(repack_body, kv_rows=kv_rows, rows=rows),
        in_specs=[ANY] + [VMEM] * len(high),
        out_specs=[VMEM] * MID,
        out_shape=[piece] * MID,
        compiler_params=pltpu.CompilerParams(vmem_limit_bytes=2 * SMALL_VMEM),
        name="repack",
    )(info, *got)
    mine = [messages[0]] + [swapped(messages[i], mid[i]) for i in range(1, MID)]
    other = [swapped(item, low[1]) for item in mine]

    if feature < HD:
        w_full = lax.dynamic_update_slice(
            jnp.zeros((HD, w_out.shape[1]), w_out.dtype), w_out, ((device * feature) % HD, 0)
        )
    else:
        w_full = w_out
    codes, scales = gate_up_codes[0], gate_up_scales[0]
    first = codes.shape[0] // 2
    gate_first, w_full = prepared([(scales, codes, 0, first)], [w_full])
    (down,) = prepared([(down_scales[0], down_codes[0], 0, down_codes.shape[1])])
    (gate_rest,) = prepared([(scales, codes, first, codes.shape[0] - first)])
    half = shards * rows // 2
    attend_vmem = 8 * 2**20 + 2 * MID * piece.size * 2 + w_full.size * 2 + half * width * 10
    keep, send = pl.pallas_call(
        functools.partial(attend_body, ctx_local=ctx_local, kv_rows=kv_rows, rows=rows),
        in_specs=[SMEM] + [VMEM] * (2 * MID + 1),
        out_specs=[VMEM] * 2,
        out_shape=[
            jax.ShapeDtypeStruct((half, width), jnp.float32),
            jax.ShapeDtypeStruct((half, width), jnp.bfloat16),
        ],
        scratch_shapes=[
            pltpu.VMEM((LOW * MID, len(high) * rows, HD), jnp.float32),
        ],
        compiler_params=pltpu.CompilerParams(vmem_limit_bytes=attend_vmem),
        name="attend",
    )(info, *mine, *other, w_full)

    projected = scatter_sum(keep, send, mid, high)
    mixed = hidden_in.astype(jnp.float32) + projected
    attention_out = mixed.astype(jnp.bfloat16)
    mean_square = jnp.mean(mixed * mixed, axis=-1, keepdims=True)
    normed = (mixed * lax.rsqrt(mean_square + EPSILON) * norm_gain).astype(jnp.bfloat16)

    experts_all = shards // 2
    hit = expert_ids[:, :, None] == jnp.arange(experts_all, dtype=jnp.int32)[None, None, :]
    combine = jnp.sum(jnp.where(hit, route_weights[:, :, None], 0.0), axis=1)
    coarse = lax.reduce_precision(combine, 8, 7)
    fine = combine - coarse
    extra = -(2 * experts_all) % HD
    tail = jnp.concatenate([coarse, fine, jnp.zeros((rows, extra), jnp.float32)], axis=1)
    held = jnp.concatenate([normed, tail.astype(jnp.bfloat16)], axis=1)
    held = joined([held] + [swapped(held, o) for o in high[1:]])
    mine = [held] + [swapped(held, o) for o in mid[1:]]
    other = [swapped(item, low[1]) for item in mine]
    expert_vmem = 4 * 2**20 + 2 * half * width * 15
    keep, send = pl.pallas_call(
        functools.partial(expert_body, width=width, experts=experts_all),
        in_specs=[VMEM] * (2 * MID + 3),
        out_specs=[VMEM] * 2,
        out_shape=[
            jax.ShapeDtypeStruct((half, width), jnp.float32),
            jax.ShapeDtypeStruct((half, width), jnp.bfloat16),
        ],
        scratch_shapes=[
            pltpu.VMEM((2 * half, width), jnp.bfloat16),
        ],
        compiler_params=pltpu.CompilerParams(vmem_limit_bytes=expert_vmem),
        name="expert",
    )(*mine, *other, gate_first, gate_rest, down)
    expert_sum = scatter_sum(keep, send, mid, high)
    layer_out = (mixed + expert_sum).astype(jnp.bfloat16)
    return (attention_out, layer_out)


def solution(mesh):
    return jax.shard_map(
        local,
        mesh=mesh,
        in_specs=(
            P(("replica", "ctx"), None),
            P(("replica", "ctx"), None),
            P(("replica", "ctx"), None),
            P("replica", "ctx", None),
            P("replica", "ctx", None),
            P("replica"),
            P("replica"),
            P(("replica", "ctx"), None),
            P("ctx", None),
            P(),
            P(("replica", "ctx"), None),
            P(("replica", "ctx"), None),
            P("ctx", None, None),
            P("ctx", None, None),
            P("ctx", None, None),
            P("ctx", None, None),
        ),
        out_specs=(P(("replica", "ctx"), None), P(("replica", "ctx"), None)),
        check_vma=False,
    )
```

```python
import functools
import math

import jax
import jax.numpy as jnp
from jax import lax
from jax.experimental import pallas as pl
from jax.experimental.pallas import tpu as pltpu
from jax.sharding import PartitionSpec as P


HD = 128
CAND = 64

NEG = -1e30
EPSILON = 1e-06
LOW = 2
MID = 4
BLK = 128
STRIP = 2**19
DEPTH = 4
SMALL_VMEM = 8 * 2**20


def swapped(value, offset):
    return lax.ppermute(value, "ctx", [(i, i ^ offset) for i in range(lax.axis_size("ctx"))])


def in_hbm(value):
    return pltpu.with_memory_space_constraint(value, pltpu.HBM)


def stage_offsets(shards):
    low = [i for i in range(LOW)]
    mid = [i * LOW for i in range(MID)]
    high = [i * LOW * MID for i in range(shards // (LOW * MID))]
    return low, mid, high


def pack_body(*refs, feature, per_group, count):
    sources, outs, held, sems = refs[:5], refs[5 : 5 + count], refs[5 + count : 10 + count], refs[10 + count]
    copies = [pltpu.make_async_copy(source, to, sems.at[i]) for i, (source, to) in enumerate(zip(sources, held))]
    for copy in copies:
        copy.start()
    for copy in copies:
        copy.wait()
    q, own_key, own_value, keys, values = held
    device = lax.axis_index("ctx")
    prefixes, ctx_local, _ = keys.shape
    rows = q.shape[0]
    kv_rows = prefixes * ctx_local

    def head_of(target):
        return (target * feature) // HD

    for zx, out in enumerate(outs):
        group = head_of(device ^ (zx * LOW * MID)) // per_group
        lanes = pl.ds(pl.multiple_of(group * HD, HD), HD)
        out[0:kv_rows, 0:HD] = keys[:, :, lanes].reshape(kv_rows, HD)
        out[0:kv_rows, HD : 2 * HD] = values[:, :, lanes].reshape(kv_rows, HD)
        for mx in range(MID):
            top = kv_rows + mx * rows
            for cx in range(LOW):
                head = head_of(device ^ (zx * LOW * MID + mx * LOW + cx))
                out[top : top + rows, cx * HD : (cx + 1) * HD] = q[:, pl.ds(pl.multiple_of(head * HD, HD), HD)]
        top = kv_rows + MID * rows
        out[top : top + rows, 0:HD] = own_key[:, lanes]
        out[top : top + rows, HD : 2 * HD] = own_value[:, lanes]


def repack_body(after, also, *refs, kv_rows, rows):
    outs = refs[-MID:]
    parts = refs[:-MID]
    for zx, part in enumerate(parts):
        for mx, out in enumerate(outs):
            out[zx, 0:kv_rows, :] = part[0:kv_rows, :]
            top = kv_rows + mx * rows
            own = kv_rows + MID * rows
            out[zx, kv_rows : kv_rows + rows, :] = part[top : top + rows, :]
            out[zx, kv_rows + rows : kv_rows + 2 * rows, :] = part[own : own + rows, :]


def attend_body(info, *refs, ctx_local, kv_rows, rows):
    mine, other = refs[:MID], refs[MID : 2 * MID]
    w_out, keep = refs[2 * MID : 2 * MID + 2]
    sends, att = refs[2 * MID + 2 : -1], refs[-1]
    device = lax.axis_index("ctx")
    high = mine[0].shape[0]
    pieces = MID * high
    span = CAND // (LOW * MID * rows)
    scale = 1.0 / math.sqrt(HD)
    tile = 2 * rows
    pick_rows = lax.broadcasted_iota(jnp.int32, (CAND, CAND * 2), 0)
    pick_cols = lax.broadcasted_iota(jnp.int32, (CAND, CAND * 2), 1)
    wanted = pick_rows // rows * tile + pick_rows % rows
    pick_query = (pick_cols == wanted).astype(jnp.bfloat16)
    pick_own = (pick_cols == wanted + rows).astype(jnp.bfloat16)
    column = lax.broadcasted_iota(jnp.int32, (CAND, pieces * ctx_local), 1)
    piece = column // ctx_local
    within = column % ctx_local
    relative = (piece % high) * (LOW * MID) + (piece // high) * LOW
    own_group = device // (LOW * MID * span)

    def joined(parts, zs, at, lanes, depth):
        return jnp.concatenate([part[zs, at, lanes].reshape(depth, -1) for part in parts], axis=0)

    for zg in range(high // span):
        prefix = info[own_group ^ zg]
        length = info[high // span + prefix]
        zs = slice(zg * span, (zg + 1) * span)
        tails = slice(kv_rows, kv_rows + tile)
        at = pl.ds(pl.multiple_of(prefix * ctx_local, ctx_local), ctx_local)
        every = slice(0, high)
        tail_mine = joined(mine, zs, tails, slice(0, 2 * HD), span * tile)
        tail_other = joined(other, zs, tails, slice(0, 2 * HD), span * tile)
        padded = jnp.concatenate([tail_mine[:, 0:HD], tail_other[:, HD : 2 * HD]], axis=0)
        query = jnp.dot(pick_query, padded, preferred_element_type=jnp.float32)
        own = jnp.dot(
            pick_own, jnp.concatenate([tail_mine, tail_other], axis=0), preferred_element_type=jnp.float32
        )
        own_score = jnp.sum(query * own[:, 0:HD], axis=1, keepdims=True) * scale
        query = query.astype(jnp.bfloat16)
        top = own_score
        all_scores = []
        for cx, source in enumerate((mine, other)):
            key = joined(source, every, at, slice(0, HD), high * ctx_local)
            scores = (
                lax.dot_general(query, key, (((1,), (1,)), ((), ())), preferred_element_type=jnp.float32) * scale
            )
            position = (device ^ (relative + cx)) * ctx_local + within
            scores = jnp.where(position < length, scores, NEG)
            top = jnp.maximum(top, jnp.max(scores, axis=1, keepdims=True))
            all_scores.append(scores)
        own_weight = jnp.exp(own_score - top)
        numer = own_weight * own[:, HD : 2 * HD]
        denom = own_weight
        for scores, source in zip(all_scores, (mine, other)):
            value = joined(source, every, at, slice(HD, 2 * HD), high * ctx_local)
            weights = jnp.exp(scores - top)
            denom = denom + jnp.sum(weights, axis=1, keepdims=True)
            numer = numer + jnp.dot(weights.astype(jnp.bfloat16), value, preferred_element_type=jnp.float32)
        attended = numer / denom
        chunk = span * rows
        att[:, zg * chunk : (zg + 1) * chunk, :] = attended.reshape(LOW * MID, chunk, HD)
    half = keep.shape[0]
    attended = att[...].reshape(2 * half, HD).astype(jnp.bfloat16)
    out = jnp.dot(attended, w_out[...], preferred_element_type=jnp.float32)
    keep[...] = out[0:half]
    for i, send in enumerate(sends):
        count = send.shape[0]
        send[...] = out[half + i * count : half + (i + 1) * count].astype(jnp.bfloat16)


def dequantize_strips(out, codes, scales, first, count, offset):
    across = codes.shape[1] // BLK
    for i in range(first, first + count):
        rows = slice(i * BLK, (i + 1) * BLK)
        for j in range(codes.shape[1] // BLK):
            lanes = slice(j * BLK, (j + 1) * BLK)
            out[rows, lanes] = (codes[rows, lanes].astype(jnp.float32) * scales[offset + i * across + j]).astype(jnp.bfloat16)


def strip_rows(shape):
    blocks = shape[0] // BLK
    count = max(1, min(blocks, STRIP // (BLK * shape[1])))
    while blocks % count:
        count -= 1
    return count * BLK


def prepare_body(*refs, ranges, fetched):
    count = len(ranges)
    scales, sources, plain = refs[0], refs[1 : 1 + count], refs[1 + count : 1 + count + fetched]
    refs = refs[1 + count + fetched :]
    outs, fetch, held, sems = refs[:count], refs[count : count + fetched], refs[count + fetched : -1], refs[-1]
    jobs = []
    for source, to, out, (start, size, base) in zip(sources, held, outs, ranges):
        step = strip_rows((size, source.shape[1]))
        for first in range(0, size, step):
            copy = pltpu.make_async_copy(
                source.at[pl.ds(start + first, step)], to.at[pl.ds(first, step)], sems.at[len(jobs)]
            )
            jobs.append((copy, (out, to, scales, first // BLK, step // BLK, base)))
    direct = [pltpu.make_async_copy(a, to, sems.at[len(jobs) + i]) for i, (a, to) in enumerate(zip(plain, fetch))]
    for copy, _ in jobs[:DEPTH]:
        copy.start()
    for copy in direct:
        copy.start()
    for i, (copy, job) in enumerate(jobs):
        copy.wait()
        if i + DEPTH < len(jobs):
            jobs[i + DEPTH][0].start()
        dequantize_strips(*job)
    for copy in direct:
        copy.wait()


def prepared(scales, weights, fetch=()):
    codes = [item[0] for item in weights]
    ranges = tuple(item[1:] for item in weights)
    fetch = list(fetch)
    shapes = [(size, a.shape[1]) for a, (_, size, _) in zip(codes, ranges)]
    steps = sum(shape[0] // strip_rows(shape) for shape in shapes)
    return pl.pallas_call(
        functools.partial(prepare_body, ranges=ranges, fetched=len(fetch)),
        in_specs=[SMEM] + [HBM] * (len(codes) + len(fetch)),
        out_specs=[VMEM] * (len(codes) + len(fetch)),
        out_shape=[pltpu.VMEM(shape, jnp.bfloat16) for shape in shapes] + [pltpu.VMEM(a.shape, a.dtype) for a in fetch],
        scratch_shapes=[pltpu.VMEM(shape, jnp.bfloat16) for shape in shapes]
        + [pltpu.SemaphoreType.DMA((steps + len(fetch),))],
        compiler_params=pltpu.CompilerParams(vmem_limit_bytes=2 * sum(math.prod(shape) for shape in shapes) + 2**20),
        name="prepare",
    )(scales, *(in_hbm(item) for item in codes + fetch))


def join_body(*refs):
    out = refs[-1]
    rows = refs[0].shape[0]
    for i, part in enumerate(refs[:-1]):
        out[i * rows : (i + 1) * rows, :] = part[...]


def joined(parts):
    rows, width = parts[0].shape
    return pl.pallas_call(
        join_body,
        in_specs=[VMEM] * len(parts),
        out_specs=VMEM,
        out_shape=jax.ShapeDtypeStruct((len(parts) * rows, width), parts[0].dtype),
        compiler_params=pltpu.CompilerParams(vmem_limit_bytes=SMALL_VMEM),
        name="join",
    )(*parts)


def expert_body(*refs, width, experts):
    parts = refs[: 2 * MID]
    gate_first, gate_rest, down, keep = refs[2 * MID : 2 * MID + 4]
    sends, x = refs[2 * MID + 4 : -1], refs[-1]
    expert = lax.axis_index("ctx") // 2
    some = parts[0].shape[0]
    half = keep.shape[0]
    for i, part in enumerate(parts):
        x[i * some : (i + 1) * some, :] = part[:, 0:width]
    tail = jnp.concatenate([part[:, width:] for part in parts], axis=0).astype(jnp.float32)
    lane = lax.broadcasted_iota(jnp.int32, tail.shape, 1)
    chosen = (lane == expert) | (lane == expert + experts)
    weight = jnp.sum(jnp.where(chosen, tail, 0.0), axis=1, keepdims=True)
    hidden = down.shape[0]
    first = gate_first.shape[0]
    act = jnp.dot(x[:, :first], gate_first[...], preferred_element_type=jnp.float32)
    act += jnp.dot(x[:, first:], gate_rest[...], preferred_element_type=jnp.float32)
    gate, up = act[:, :hidden], act[:, hidden:]
    active = (gate / (1.0 + jnp.exp(-gate)) * up).astype(jnp.bfloat16)
    out = jnp.dot(active, down[...], preferred_element_type=jnp.float32) * weight
    keep[...] = out[0:half]
    for i, send in enumerate(sends):
        count = send.shape[0]
        send[...] = out[half + i * count : half + (i + 1) * count].astype(jnp.bfloat16)


VMEM = pl.BlockSpec(memory_space=pltpu.VMEM)
SMEM = pl.BlockSpec(memory_space=pltpu.SMEM)
HBM = pl.BlockSpec(memory_space=pltpu.HBM)
ANY = pl.BlockSpec(memory_space=pl.ANY)


def add_body(keep, got, out, *, first):
    out[...] = (keep[first : first + out.shape[0], :] + got[...].astype(jnp.float32)).astype(out.dtype)


def added(keep, got, first):
    return pl.pallas_call(
        functools.partial(add_body, first=first),
        in_specs=[VMEM] * 2,
        out_specs=VMEM,
        out_shape=jax.ShapeDtypeStruct(got.shape, got.dtype),
        compiler_params=pltpu.CompilerParams(vmem_limit_bytes=keep.size * 4 + got.size * 8 + 2**20),
        name="add",
    )(keep, got)


def scatter_sum(keep, sends, mid, high):
    width = keep.shape[1]
    step = sends[0].shape[0]
    order = (*range(1, len(mid)), 0)
    came = {i: swapped(sends[i], 1) for i in order}
    total = keep[:step] + came[0].astype(jnp.float32)
    got = [swapped(added(keep, came[i], i * step), mid[i]) for i in order[:-1]]
    for item in got:
        total = total + item.astype(jnp.float32)
    parts = total.reshape(len(high), -1, width)
    total = parts[0]
    got = [swapped(parts[i].astype(jnp.bfloat16), high[i]) for i in range(1, len(high))]
    for item in got:
        total = total + item.astype(jnp.float32)
    return total


def local(
    queries,
    own_key,
    own_value,
    cache_keys,
    cache_values,
    prefix_of_row,
    context_len,
    hidden_in,
    w_out,
    norm_gain,
    expert_ids,
    route_weights,
    gate_up_codes,
    gate_up_scales,
    down_codes,
    down_scales,
):
    shards = lax.axis_size("ctx")
    device = lax.axis_index("ctx")
    rows = queries.shape[0]
    width = hidden_in.shape[1]
    key_groups = own_key.shape[1] // HD
    head_count = queries.shape[1] // HD
    per_group = head_count // key_groups
    prefixes, ctx_local, _ = cache_keys.shape
    kv_rows = prefixes * ctx_local
    feature = w_out.shape[0]
    low, mid, high = stage_offsets(shards)
    info = jnp.concatenate([prefix_of_row[::CAND], context_len])
    scales = jnp.concatenate([gate_up_scales.reshape(-1), down_scales.reshape(-1)])

    inputs = (queries, own_key, own_value, cache_keys, cache_values)
    message = jax.ShapeDtypeStruct((kv_rows + MID * rows + 2 * rows, 2 * HD), jnp.bfloat16)
    messages = pl.pallas_call(
        functools.partial(pack_body, feature=feature, per_group=per_group, count=len(high)),
        in_specs=[HBM] * len(inputs),
        out_specs=[VMEM] * len(high),
        out_shape=[message] * len(high),
        scratch_shapes=[pltpu.VMEM(a.shape, a.dtype) for a in inputs] + [pltpu.SemaphoreType.DMA((len(inputs),))],
        compiler_params=pltpu.CompilerParams(vmem_limit_bytes=SMALL_VMEM),
        name="pack",
    )(*(in_hbm(item) for item in inputs))
    got = [messages[0]] + [swapped(messages[i], high[i]) for i in range(1, len(high))]
    piece = jax.ShapeDtypeStruct((len(high), kv_rows + 2 * rows, 2 * HD), jnp.bfloat16)
    messages = pl.pallas_call(
        functools.partial(repack_body, kv_rows=kv_rows, rows=rows),
        in_specs=[ANY] * 2 + [VMEM] * len(high),
        out_specs=[VMEM] * MID,
        out_shape=[piece] * MID,
        compiler_params=pltpu.CompilerParams(vmem_limit_bytes=2 * SMALL_VMEM),
        name="repack",
    )(info, scales, *got)
    mine = [messages[0]] + [swapped(messages[i], mid[i]) for i in range(1, MID)]
    other = [swapped(item, low[1]) for item in mine]

    if feature < HD:
        w_full = lax.dynamic_update_slice(
            jnp.zeros((HD, w_out.shape[1]), w_out.dtype), w_out, ((device * feature) % HD, 0)
        )
    else:
        w_full = w_out
    codes = gate_up_codes[0]
    first = codes.shape[0] // 2
    gate_first, w_full = prepared(scales, [(codes, 0, first, 0)], [w_full])
    (down,) = prepared(scales, [(down_codes[0], 0, down_codes.shape[1], gate_up_scales.size)])
    (gate_rest,) = prepared(scales, [(codes, first, codes.shape[0] - first, first // BLK * gate_up_scales.shape[2])])
    half = shards * rows // 2
    attend_vmem = 8 * 2**20 + 2 * MID * piece.size * 2 + w_full.size * 2 + half * width * 10
    keep, *sends = pl.pallas_call(
        functools.partial(attend_body, ctx_local=ctx_local, kv_rows=kv_rows, rows=rows),
        in_specs=[SMEM] + [VMEM] * (2 * MID + 1),
        out_specs=[VMEM] * (1 + MID),
        out_shape=[
            jax.ShapeDtypeStruct((half, width), jnp.float32),
            *[jax.ShapeDtypeStruct((half // MID, width), jnp.bfloat16)] * MID,
        ],
        scratch_shapes=[
            pltpu.VMEM((LOW * MID, len(high) * rows, HD), jnp.float32),
        ],
        compiler_params=pltpu.CompilerParams(vmem_limit_bytes=attend_vmem),
        name="attend",
    )(info, *mine, *other, w_full)

    projected = scatter_sum(keep, sends, mid, high)
    mixed = hidden_in.astype(jnp.float32) + projected
    attention_out = mixed.astype(jnp.bfloat16)
    mean_square = jnp.mean(mixed * mixed, axis=-1, keepdims=True)
    normed = (mixed * lax.rsqrt(mean_square + EPSILON) * norm_gain).astype(jnp.bfloat16)

    experts_all = shards // 2
    hit = expert_ids[:, :, None] == jnp.arange(experts_all, dtype=jnp.int32)[None, None, :]
    combine = jnp.sum(jnp.where(hit, route_weights[:, :, None], 0.0), axis=1)
    coarse = lax.reduce_precision(combine, 8, 7)
    fine = combine - coarse
    extra = -(2 * experts_all) % HD
    tail = jnp.concatenate([coarse, fine, jnp.zeros((rows, extra), jnp.float32)], axis=1)
    held = jnp.concatenate([normed, tail.astype(jnp.bfloat16)], axis=1)
    held = joined([held] + [swapped(held, o) for o in high[1:]])
    mine = [held] + [swapped(held, o) for o in mid[1:]]
    other = [swapped(item, low[1]) for item in mine]
    expert_vmem = 4 * 2**20 + 2 * half * width * 15
    keep, *sends = pl.pallas_call(
        functools.partial(expert_body, width=width, experts=experts_all),
        in_specs=[VMEM] * (2 * MID + 3),
        out_specs=[VMEM] * (1 + MID),
        out_shape=[
            jax.ShapeDtypeStruct((half, width), jnp.float32),
            *[jax.ShapeDtypeStruct((half // MID, width), jnp.bfloat16)] * MID,
        ],
        scratch_shapes=[
            pltpu.VMEM((2 * half, width), jnp.bfloat16),
        ],
        compiler_params=pltpu.CompilerParams(vmem_limit_bytes=expert_vmem),
        name="expert",
    )(*mine, *other, gate_first, gate_rest, down)
    expert_sum = scatter_sum(keep, sends, mid, high)
    layer_out = (mixed + expert_sum).astype(jnp.bfloat16)
    return (attention_out, layer_out)


def solution(mesh):
    return jax.shard_map(
        local,
        mesh=mesh,
        in_specs=(
            P(("replica", "ctx"), None),
            P(("replica", "ctx"), None),
            P(("replica", "ctx"), None),
            P("replica", "ctx", None),
            P("replica", "ctx", None),
            P("replica"),
            P("replica"),
            P(("replica", "ctx"), None),
            P("ctx", None),
            P(),
            P(("replica", "ctx"), None),
            P(("replica", "ctx"), None),
            P("ctx", None, None),
            P("ctx", None, None),
            P("ctx", None, None),
            P("ctx", None, None),
        ),
        out_specs=(P(("replica", "ctx"), None), P(("replica", "ctx"), None)),
        check_vma=False,
    )
```

```python
import functools
import math

import jax
import jax.numpy as jnp
from jax import lax
from jax.experimental import pallas as pl
from jax.experimental.pallas import tpu as pltpu
from jax.sharding import PartitionSpec as P


HD = 128
CAND = 64

NEG = -1e30
EPSILON = 1e-06
LOW = 2
MID = 4
BLK = 128
STRIP = 2**19
DEPTH = 4
SMALL_VMEM = 8 * 2**20


def swapped(value, offset):
    return lax.ppermute(value, "ctx", [(i, i ^ offset) for i in range(lax.axis_size("ctx"))])


def in_hbm(value):
    return pltpu.with_memory_space_constraint(value, pltpu.HBM)


def stage_offsets(shards):
    low = [i for i in range(LOW)]
    mid = [i * LOW for i in range(MID)]
    high = [i * LOW * MID for i in range(shards // (LOW * MID))]
    return low, mid, high


def pack_body(*refs, feature, per_group, count, tables):
    sources, refs = refs[: 5 + tables], refs[5 + tables :]
    outs, kept, held, sems = refs[:count], refs[count : count + tables], refs[count + tables : -1], refs[-1]
    goals = (*held, *kept)
    copies = [pltpu.make_async_copy(source, to, sems.at[i]) for i, (source, to) in enumerate(zip(sources, goals))]
    for copy in copies:
        copy.start()
    for copy in copies:
        copy.wait()
    q, own_key, own_value, keys, values = held
    device = lax.axis_index("ctx")
    prefixes, ctx_local, _ = keys.shape
    rows = q.shape[0]
    kv_rows = prefixes * ctx_local

    def head_of(target):
        return (target * feature) // HD

    for zx, out in enumerate(outs):
        group = head_of(device ^ (zx * LOW * MID)) // per_group
        lanes = pl.ds(pl.multiple_of(group * HD, HD), HD)
        out[0:kv_rows, 0:HD] = keys[:, :, lanes].reshape(kv_rows, HD)
        out[0:kv_rows, HD : 2 * HD] = values[:, :, lanes].reshape(kv_rows, HD)
        for mx in range(MID):
            top = kv_rows + mx * rows
            for cx in range(LOW):
                head = head_of(device ^ (zx * LOW * MID + mx * LOW + cx))
                out[top : top + rows, cx * HD : (cx + 1) * HD] = q[:, pl.ds(pl.multiple_of(head * HD, HD), HD)]
        top = kv_rows + MID * rows
        out[top : top + rows, 0:HD] = own_key[:, lanes]
        out[top : top + rows, HD : 2 * HD] = own_value[:, lanes]


def repack_body(*refs, kv_rows, rows):
    outs = refs[-MID:]
    parts = refs[:-MID]
    for zx, part in enumerate(parts):
        for mx, out in enumerate(outs):
            out[zx, 0:kv_rows, :] = part[0:kv_rows, :]
            top = kv_rows + mx * rows
            own = kv_rows + MID * rows
            out[zx, kv_rows : kv_rows + rows, :] = part[top : top + rows, :]
            out[zx, kv_rows + rows : kv_rows + 2 * rows, :] = part[own : own + rows, :]


def attend_body(prefix_of, lengths, *refs, ctx_local, kv_rows, rows):
    mine, other = refs[:MID], refs[MID : 2 * MID]
    w_out, keep = refs[2 * MID : 2 * MID + 2]
    sends, att = refs[2 * MID + 2 : -1], refs[-1]
    device = lax.axis_index("ctx")
    high = mine[0].shape[0]
    pieces = MID * high
    span = CAND // (LOW * MID * rows)
    scale = 1.0 / math.sqrt(HD)
    tile = 2 * rows
    pick_rows = lax.broadcasted_iota(jnp.int32, (CAND, CAND * 2), 0)
    pick_cols = lax.broadcasted_iota(jnp.int32, (CAND, CAND * 2), 1)
    wanted = pick_rows // rows * tile + pick_rows % rows
    pick_query = (pick_cols == wanted).astype(jnp.bfloat16)
    pick_own = (pick_cols == wanted + rows).astype(jnp.bfloat16)
    column = lax.broadcasted_iota(jnp.int32, (CAND, pieces * ctx_local), 1)
    piece = column // ctx_local
    within = column % ctx_local
    relative = (piece % high) * (LOW * MID) + (piece // high) * LOW
    own_group = device // (LOW * MID * span)

    def joined(parts, zs, at, lanes, depth):
        return jnp.concatenate([part[zs, at, lanes].reshape(depth, -1) for part in parts], axis=0)

    for zg in range(high // span):
        prefix = prefix_of[(own_group ^ zg) * CAND]
        length = lengths[prefix]
        zs = slice(zg * span, (zg + 1) * span)
        tails = slice(kv_rows, kv_rows + tile)
        at = pl.ds(pl.multiple_of(prefix * ctx_local, ctx_local), ctx_local)
        every = slice(0, high)
        tail_mine = joined(mine, zs, tails, slice(0, 2 * HD), span * tile)
        tail_other = joined(other, zs, tails, slice(0, 2 * HD), span * tile)
        padded = jnp.concatenate([tail_mine[:, 0:HD], tail_other[:, HD : 2 * HD]], axis=0)
        query = jnp.dot(pick_query, padded, preferred_element_type=jnp.float32)
        own = jnp.dot(
            pick_own, jnp.concatenate([tail_mine, tail_other], axis=0), preferred_element_type=jnp.float32
        )
        own_score = jnp.sum(query * own[:, 0:HD], axis=1, keepdims=True) * scale
        query = query.astype(jnp.bfloat16)
        top = own_score
        all_scores = []
        for cx, source in enumerate((mine, other)):
            key = joined(source, every, at, slice(0, HD), high * ctx_local)
            scores = (
                lax.dot_general(query, key, (((1,), (1,)), ((), ())), preferred_element_type=jnp.float32) * scale
            )
            position = (device ^ (relative + cx)) * ctx_local + within
            scores = jnp.where(position < length, scores, NEG)
            top = jnp.maximum(top, jnp.max(scores, axis=1, keepdims=True))
            all_scores.append(scores)
        own_weight = jnp.exp(own_score - top)
        numer = own_weight * own[:, HD : 2 * HD]
        denom = own_weight
        for scores, source in zip(all_scores, (mine, other)):
            value = joined(source, every, at, slice(HD, 2 * HD), high * ctx_local)
            weights = jnp.exp(scores - top)
            denom = denom + jnp.sum(weights, axis=1, keepdims=True)
            numer = numer + jnp.dot(weights.astype(jnp.bfloat16), value, preferred_element_type=jnp.float32)
        attended = numer / denom
        chunk = span * rows
        att[:, zg * chunk : (zg + 1) * chunk, :] = attended.reshape(LOW * MID, chunk, HD)
    half = keep.shape[0]
    attended = att[...].reshape(2 * half, HD).astype(jnp.bfloat16)
    out = jnp.dot(attended, w_out[...], preferred_element_type=jnp.float32)
    keep[...] = out[0:half]
    for i, send in enumerate(sends):
        count = send.shape[0]
        send[...] = out[half + i * count : half + (i + 1) * count].astype(jnp.bfloat16)


def dequantize_strips(out, codes, scales, across, first, count, offset):
    for i in range(first, first + count):
        rows = slice(i * BLK, (i + 1) * BLK)
        for j in range(codes.shape[1] // BLK):
            lanes = slice(j * BLK, (j + 1) * BLK)
            scale = scales[j, 0, offset + i] if across else scales[offset + i, 0, j]
            out[rows, lanes] = (codes[rows, lanes].astype(jnp.float32) * scale).astype(jnp.bfloat16)


def strip_rows(shape):
    blocks = shape[0] // BLK
    count = max(1, min(blocks, STRIP // (BLK * shape[1])))
    while blocks % count:
        count -= 1
    return count * BLK


def prepare_body(*refs, ranges, fetched, across):
    count = len(ranges)
    scales, sources, plain = refs[0], refs[1 : 1 + count], refs[1 + count : 1 + count + fetched]
    refs = refs[1 + count + fetched :]
    outs, fetch, held, sems = refs[:count], refs[count : count + fetched], refs[count + fetched : -1], refs[-1]
    jobs = []
    for source, to, out, (start, size) in zip(sources, held, outs, ranges):
        step = strip_rows((size, source.shape[1]))
        for first in range(0, size, step):
            copy = pltpu.make_async_copy(
                source.at[pl.ds(start + first, step)], to.at[pl.ds(first, step)], sems.at[len(jobs)]
            )
            jobs.append((copy, (out, to, scales, across, first // BLK, step // BLK, start // BLK)))
    direct = [pltpu.make_async_copy(a, to, sems.at[len(jobs) + i]) for i, (a, to) in enumerate(zip(plain, fetch))]
    for copy, _ in jobs[:DEPTH]:
        copy.start()
    for copy in direct:
        copy.start()
    for i, (copy, job) in enumerate(jobs):
        copy.wait()
        if i + DEPTH < len(jobs):
            jobs[i + DEPTH][0].start()
        dequantize_strips(*job)
    for copy in direct:
        copy.wait()


def prepared(scales, across, weights, fetch=()):
    codes = [item[0] for item in weights]
    ranges = tuple(item[1:] for item in weights)
    fetch = list(fetch)
    shapes = [(size, a.shape[1]) for a, (_, size) in zip(codes, ranges)]
    steps = sum(shape[0] // strip_rows(shape) for shape in shapes)
    return pl.pallas_call(
        functools.partial(prepare_body, ranges=ranges, fetched=len(fetch), across=across),
        in_specs=[SMEM] + [HBM] * (len(codes) + len(fetch)),
        out_specs=[VMEM] * (len(codes) + len(fetch)),
        out_shape=[pltpu.VMEM(shape, jnp.bfloat16) for shape in shapes] + [pltpu.VMEM(a.shape, a.dtype) for a in fetch],
        scratch_shapes=[pltpu.VMEM(shape, jnp.bfloat16) for shape in shapes]
        + [pltpu.SemaphoreType.DMA((steps + len(fetch),))],
        compiler_params=pltpu.CompilerParams(vmem_limit_bytes=2 * sum(math.prod(shape) for shape in shapes) + 2**20),
        name="prepare",
    )(scales, *(in_hbm(item) for item in codes + fetch))


def join_body(*refs):
    out = refs[-1]
    rows = refs[0].shape[0]
    for i, part in enumerate(refs[:-1]):
        out[i * rows : (i + 1) * rows, :] = part[...]


def joined(parts):
    rows, width = parts[0].shape
    return pl.pallas_call(
        join_body,
        in_specs=[VMEM] * len(parts),
        out_specs=VMEM,
        out_shape=jax.ShapeDtypeStruct((len(parts) * rows, width), parts[0].dtype),
        compiler_params=pltpu.CompilerParams(vmem_limit_bytes=SMALL_VMEM),
        name="join",
    )(*parts)


def expert_body(*refs, width, experts):
    parts = refs[: 2 * MID]
    gate_first, gate_rest, down, keep = refs[2 * MID : 2 * MID + 4]
    sends, x = refs[2 * MID + 4 : -1], refs[-1]
    expert = lax.axis_index("ctx") // 2
    some = parts[0].shape[0]
    half = keep.shape[0]
    for i, part in enumerate(parts):
        x[i * some : (i + 1) * some, :] = part[:, 0:width]
    tail = jnp.concatenate([part[:, width:] for part in parts], axis=0).astype(jnp.float32)
    lane = lax.broadcasted_iota(jnp.int32, tail.shape, 1)
    chosen = (lane == expert) | (lane == expert + experts)
    weight = jnp.sum(jnp.where(chosen, tail, 0.0), axis=1, keepdims=True)
    hidden = down.shape[0]
    first = gate_first.shape[0]
    act = jnp.dot(x[:, :first], gate_first[...], preferred_element_type=jnp.float32)
    act += jnp.dot(x[:, first:], gate_rest[...], preferred_element_type=jnp.float32)
    gate, up = act[:, :hidden], act[:, hidden:]
    active = (gate / (1.0 + jnp.exp(-gate)) * up).astype(jnp.bfloat16)
    out = jnp.dot(active, down[...], preferred_element_type=jnp.float32) * weight
    keep[...] = out[0:half]
    for i, send in enumerate(sends):
        count = send.shape[0]
        send[...] = out[half + i * count : half + (i + 1) * count].astype(jnp.bfloat16)


VMEM = pl.BlockSpec(memory_space=pltpu.VMEM)
SMEM = pl.BlockSpec(memory_space=pltpu.SMEM)
HBM = pl.BlockSpec(memory_space=pltpu.HBM)
ANY = pl.BlockSpec(memory_space=pl.ANY)


def add_body(keep, got, out, *, first):
    out[...] = (keep[first : first + out.shape[0], :] + got[...].astype(jnp.float32)).astype(out.dtype)


def added(keep, got, first):
    return pl.pallas_call(
        functools.partial(add_body, first=first),
        in_specs=[VMEM] * 2,
        out_specs=VMEM,
        out_shape=jax.ShapeDtypeStruct(got.shape, got.dtype),
        compiler_params=pltpu.CompilerParams(vmem_limit_bytes=keep.size * 4 + got.size * 8 + 2**20),
        name="add",
    )(keep, got)


def scatter_sum(keep, sends, mid, high):
    width = keep.shape[1]
    step = sends[0].shape[0]
    order = (*range(1, len(mid)), 0)
    came = {i: swapped(sends[i], 1) for i in order}
    total = keep[:step] + came[0].astype(jnp.float32)
    got = [swapped(added(keep, came[i], i * step), mid[i]) for i in order[:-1]]
    for item in got:
        total = total + item.astype(jnp.float32)
    parts = total.reshape(len(high), -1, width)
    total = parts[0]
    got = [swapped(parts[i].astype(jnp.bfloat16), high[i]) for i in range(1, len(high))]
    for item in got:
        total = total + item.astype(jnp.float32)
    return total


def local(
    queries,
    own_key,
    own_value,
    cache_keys,
    cache_values,
    prefix_of_row,
    context_len,
    hidden_in,
    w_out,
    norm_gain,
    expert_ids,
    route_weights,
    gate_up_codes,
    gate_up_scales,
    down_codes,
    down_scales,
):
    shards = lax.axis_size("ctx")
    device = lax.axis_index("ctx")
    rows = queries.shape[0]
    width = hidden_in.shape[1]
    key_groups = own_key.shape[1] // HD
    head_count = queries.shape[1] // HD
    per_group = head_count // key_groups
    prefixes, ctx_local, _ = cache_keys.shape
    kv_rows = prefixes * ctx_local
    feature = w_out.shape[0]
    low, mid, high = stage_offsets(shards)
    tables = (prefix_of_row, context_len, gate_up_scales.transpose(2, 0, 1), down_scales.transpose(1, 0, 2))

    inputs = (queries, own_key, own_value, cache_keys, cache_values)
    message = jax.ShapeDtypeStruct((kv_rows + MID * rows + 2 * rows, 2 * HD), jnp.bfloat16)
    steps = len(inputs) + len(tables)
    packed = pl.pallas_call(
        functools.partial(pack_body, feature=feature, per_group=per_group, count=len(high), tables=len(tables)),
        in_specs=[HBM] * steps,
        out_specs=[VMEM] * (len(high) + len(tables)),
        out_shape=[message] * len(high) + [jax.ShapeDtypeStruct(a.shape, a.dtype) for a in tables],
        scratch_shapes=[pltpu.VMEM(a.shape, a.dtype) for a in inputs] + [pltpu.SemaphoreType.DMA((steps,))],
        compiler_params=pltpu.CompilerParams(vmem_limit_bytes=SMALL_VMEM),
        name="pack",
    )(*(in_hbm(item) for item in inputs + tables))
    messages, (prefix_of, lengths, gate_scales, low_scales) = packed[: len(high)], packed[len(high) :]
    got = [messages[0]] + [swapped(messages[i], high[i]) for i in range(1, len(high))]
    piece = jax.ShapeDtypeStruct((len(high), kv_rows + 2 * rows, 2 * HD), jnp.bfloat16)
    messages = pl.pallas_call(
        functools.partial(repack_body, kv_rows=kv_rows, rows=rows),
        in_specs=[VMEM] * len(high),
        out_specs=[VMEM] * MID,
        out_shape=[piece] * MID,
        compiler_params=pltpu.CompilerParams(vmem_limit_bytes=2 * SMALL_VMEM),
        name="repack",
    )(*got)
    mine = [messages[0]] + [swapped(messages[i], mid[i]) for i in range(1, MID)]
    other = [swapped(item, low[1]) for item in mine]

    if feature < HD:
        w_full = lax.dynamic_update_slice(
            jnp.zeros((HD, w_out.shape[1]), w_out.dtype), w_out, ((device * feature) % HD, 0)
        )
    else:
        w_full = w_out
    codes = gate_up_codes[0]
    first = codes.shape[0] // 2
    gate_first, w_full = prepared(gate_scales, True, [(codes, 0, first)], [w_full])
    (down,) = prepared(low_scales, False, [(down_codes[0], 0, down_codes.shape[1])])
    (gate_rest,) = prepared(gate_scales, True, [(codes, first, codes.shape[0] - first)])
    half = shards * rows // 2
    attend_vmem = 8 * 2**20 + 2 * MID * piece.size * 2 + w_full.size * 2 + half * width * 10
    keep, *sends = pl.pallas_call(
        functools.partial(attend_body, ctx_local=ctx_local, kv_rows=kv_rows, rows=rows),
        in_specs=[SMEM] * 2 + [VMEM] * (2 * MID + 1),
        out_specs=[VMEM] * (1 + MID),
        out_shape=[
            jax.ShapeDtypeStruct((half, width), jnp.float32),
            *[jax.ShapeDtypeStruct((half // MID, width), jnp.bfloat16)] * MID,
        ],
        scratch_shapes=[
            pltpu.VMEM((LOW * MID, len(high) * rows, HD), jnp.float32),
        ],
        compiler_params=pltpu.CompilerParams(vmem_limit_bytes=attend_vmem),
        name="attend",
    )(prefix_of, lengths, *mine, *other, w_full)

    projected = scatter_sum(keep, sends, mid, high)
    mixed = hidden_in.astype(jnp.float32) + projected
    attention_out = mixed.astype(jnp.bfloat16)
    mean_square = jnp.mean(mixed * mixed, axis=-1, keepdims=True)
    normed = (mixed * lax.rsqrt(mean_square + EPSILON) * norm_gain).astype(jnp.bfloat16)

    experts_all = shards // 2
    hit = expert_ids[:, :, None] == jnp.arange(experts_all, dtype=jnp.int32)[None, None, :]
    combine = jnp.sum(jnp.where(hit, route_weights[:, :, None], 0.0), axis=1)
    coarse = lax.reduce_precision(combine, 8, 7)
    fine = combine - coarse
    extra = -(2 * experts_all) % HD
    tail = jnp.concatenate([coarse, fine, jnp.zeros((rows, extra), jnp.float32)], axis=1)
    held = jnp.concatenate([normed, tail.astype(jnp.bfloat16)], axis=1)
    held = joined([held] + [swapped(held, o) for o in high[1:]])
    mine = [held] + [swapped(held, o) for o in mid[1:]]
    other = [swapped(item, low[1]) for item in mine]
    expert_vmem = 4 * 2**20 + 2 * half * width * 15
    keep, *sends = pl.pallas_call(
        functools.partial(expert_body, width=width, experts=experts_all),
        in_specs=[VMEM] * (2 * MID + 3),
        out_specs=[VMEM] * (1 + MID),
        out_shape=[
            jax.ShapeDtypeStruct((half, width), jnp.float32),
            *[jax.ShapeDtypeStruct((half // MID, width), jnp.bfloat16)] * MID,
        ],
        scratch_shapes=[
            pltpu.VMEM((2 * half, width), jnp.bfloat16),
        ],
        compiler_params=pltpu.CompilerParams(vmem_limit_bytes=expert_vmem),
        name="expert",
    )(*mine, *other, gate_first, gate_rest, down)
    expert_sum = scatter_sum(keep, sends, mid, high)
    layer_out = (mixed + expert_sum).astype(jnp.bfloat16)
    return (attention_out, layer_out)


def solution(mesh):
    return jax.shard_map(
        local,
        mesh=mesh,
        in_specs=(
            P(("replica", "ctx"), None),
            P(("replica", "ctx"), None),
            P(("replica", "ctx"), None),
            P("replica", "ctx", None),
            P("replica", "ctx", None),
            P("replica"),
            P("replica"),
            P(("replica", "ctx"), None),
            P("ctx", None),
            P(),
            P(("replica", "ctx"), None),
            P(("replica", "ctx"), None),
            P("ctx", None, None),
            P("ctx", None, None),
            P("ctx", None, None),
            P("ctx", None, None),
        ),
        out_specs=(P(("replica", "ctx"), None), P(("replica", "ctx"), None)),
        check_vma=False,
    )
```

```python
import functools
import math

import jax
import jax.numpy as jnp
from jax import lax
from jax.experimental import pallas as pl
from jax.experimental.pallas import tpu as pltpu
from jax.sharding import PartitionSpec as P


HD = 128
CAND = 64

NEG = -1e30
EPSILON = 1e-06
LOW = 2
MID = 4
BLK = 128
STRIP = 2**19
DEPTH = 4
SMALL_VMEM = 8 * 2**20


def swapped(value, offset):
    return lax.ppermute(value, "ctx", [(i, i ^ offset) for i in range(lax.axis_size("ctx"))])


def in_hbm(value):
    return pltpu.with_memory_space_constraint(value, pltpu.HBM)


def stage_offsets(shards):
    low = [i for i in range(LOW)]
    mid = [i * LOW for i in range(MID)]
    high = [i * LOW * MID for i in range(shards // (LOW * MID))]
    return low, mid, high


def pack_body(*refs, feature, per_group, count, tables):
    sources, refs = refs[: 5 + tables], refs[5 + tables :]
    outs, kept, held, sems = refs[:count], refs[count : count + tables], refs[count + tables : -1], refs[-1]
    goals = (*held, *kept)
    copies = [pltpu.make_async_copy(source, to, sems.at[i]) for i, (source, to) in enumerate(zip(sources, goals))]
    for copy in copies:
        copy.start()
    for copy in copies:
        copy.wait()
    q, own_key, own_value, keys, values = held
    device = lax.axis_index("ctx")
    prefixes, ctx_local, _ = keys.shape
    rows = q.shape[0]
    kv_rows = prefixes * ctx_local

    def head_of(target):
        return (target * feature) // HD

    def fill(out, zx, middle, own):
        group = head_of(device ^ (zx * LOW * MID)) // per_group
        lanes = pl.ds(pl.multiple_of(group * HD, HD), HD)
        out[0:kv_rows, 0:HD] = keys[:, :, lanes].reshape(kv_rows, HD)
        out[0:kv_rows, HD : 2 * HD] = values[:, :, lanes].reshape(kv_rows, HD)
        for i, mx in enumerate(middle):
            top = kv_rows + i * rows
            for cx in range(LOW):
                head = head_of(device ^ (zx * LOW * MID + mx * LOW + cx))
                out[top : top + rows, cx * HD : (cx + 1) * HD] = q[:, pl.ds(pl.multiple_of(head * HD, HD), HD)]
        out[own : own + rows, 0:HD] = own_key[:, lanes]
        out[own : own + rows, HD : 2 * HD] = own_value[:, lanes]

    for mx in range(MID):
        fill(outs[mx], 0, [mx], kv_rows + rows)
    for zx, out in enumerate(outs[MID:], 1):
        fill(out, zx, range(MID), kv_rows + MID * rows)


def repack_body(*refs, kv_rows, rows):
    outs = refs[-MID:]
    parts = refs[:-MID]
    for zx, part in enumerate(parts):
        for mx, out in enumerate(outs):
            out[zx, 0:kv_rows, :] = part[0:kv_rows, :]
            top = kv_rows + mx * rows
            own = kv_rows + MID * rows
            out[zx, kv_rows : kv_rows + rows, :] = part[top : top + rows, :]
            out[zx, kv_rows + rows : kv_rows + 2 * rows, :] = part[own : own + rows, :]


def attend_body(prefix_of, lengths, *refs, ctx_local, kv_rows, rows):
    mine, other = (list(zip(part[:MID], part[MID:])) for part in (refs[: 2 * MID], refs[2 * MID : 4 * MID]))
    w_out, keep = refs[4 * MID : 4 * MID + 2]
    sends, att = refs[4 * MID + 2 : -1], refs[-1]
    device = lax.axis_index("ctx")
    high = mine[0][1].shape[0] + 1
    pieces = MID * high
    span = CAND // (LOW * MID * rows)
    scale = 1.0 / math.sqrt(HD)
    tile = 2 * rows
    pick_rows = lax.broadcasted_iota(jnp.int32, (CAND, CAND * 2), 0)
    pick_cols = lax.broadcasted_iota(jnp.int32, (CAND, CAND * 2), 1)
    wanted = pick_rows // rows * tile + pick_rows % rows
    pick_query = (pick_cols == wanted).astype(jnp.bfloat16)
    pick_own = (pick_cols == wanted + rows).astype(jnp.bfloat16)
    column = lax.broadcasted_iota(jnp.int32, (CAND, pieces * ctx_local), 1)
    piece = column // ctx_local
    within = column % ctx_local
    relative = (piece % high) * (LOW * MID) + (piece // high) * LOW
    own_group = device // (LOW * MID * span)

    def joined(parts, zs, at, lanes):
        taken = []
        for near, rest in parts:
            first, last = zs.start, zs.stop
            if first == 0:
                taken.append(near[at, lanes])
                first = 1
            block = rest[first - 1 : last - 1, at, lanes]
            taken.append(block.reshape(-1, block.shape[-1]))
        return jnp.concatenate(taken, axis=0)

    for zg in range(high // span):
        prefix = prefix_of[(own_group ^ zg) * CAND]
        length = lengths[prefix]
        zs = slice(zg * span, (zg + 1) * span)
        tails = slice(kv_rows, kv_rows + tile)
        at = pl.ds(pl.multiple_of(prefix * ctx_local, ctx_local), ctx_local)
        every = slice(0, high)
        tail_mine = joined(mine, zs, tails, slice(0, 2 * HD))
        tail_other = joined(other, zs, tails, slice(0, 2 * HD))
        padded = jnp.concatenate([tail_mine[:, 0:HD], tail_other[:, HD : 2 * HD]], axis=0)
        query = jnp.dot(pick_query, padded, preferred_element_type=jnp.float32)
        own = jnp.dot(
            pick_own, jnp.concatenate([tail_mine, tail_other], axis=0), preferred_element_type=jnp.float32
        )
        own_score = jnp.sum(query * own[:, 0:HD], axis=1, keepdims=True) * scale
        query = query.astype(jnp.bfloat16)
        top = own_score
        all_scores = []
        for cx, source in enumerate((mine, other)):
            key = joined(source, every, at, slice(0, HD))
            scores = (
                lax.dot_general(query, key, (((1,), (1,)), ((), ())), preferred_element_type=jnp.float32) * scale
            )
            position = (device ^ (relative + cx)) * ctx_local + within
            scores = jnp.where(position < length, scores, NEG)
            top = jnp.maximum(top, jnp.max(scores, axis=1, keepdims=True))
            all_scores.append(scores)
        own_weight = jnp.exp(own_score - top)
        numer = own_weight * own[:, HD : 2 * HD]
        denom = own_weight
        for scores, source in zip(all_scores, (mine, other)):
            value = joined(source, every, at, slice(HD, 2 * HD))
            weights = jnp.exp(scores - top)
            denom = denom + jnp.sum(weights, axis=1, keepdims=True)
            numer = numer + jnp.dot(weights.astype(jnp.bfloat16), value, preferred_element_type=jnp.float32)
        attended = numer / denom
        chunk = span * rows
        att[:, zg * chunk : (zg + 1) * chunk, :] = attended.reshape(LOW * MID, chunk, HD)
    half = keep.shape[0]
    attended = att[...].reshape(2 * half, HD).astype(jnp.bfloat16)
    out = jnp.dot(attended, w_out[...], preferred_element_type=jnp.float32)
    keep[...] = out[0:half]
    for i, send in enumerate(sends):
        count = send.shape[0]
        send[...] = out[half + i * count : half + (i + 1) * count].astype(jnp.bfloat16)


def dequantize_strips(out, codes, scales, across, first, count, offset):
    for i in range(first, first + count):
        rows = slice(i * BLK, (i + 1) * BLK)
        for j in range(codes.shape[1] // BLK):
            lanes = slice(j * BLK, (j + 1) * BLK)
            scale = scales[j, 0, offset + i] if across else scales[offset + i, 0, j]
            out[rows, lanes] = (codes[rows, lanes].astype(jnp.float32) * scale).astype(jnp.bfloat16)


def strip_rows(shape):
    blocks = shape[0] // BLK
    count = max(1, min(blocks, STRIP // (BLK * shape[1])))
    while blocks % count:
        count -= 1
    return count * BLK


def prepare_body(*refs, ranges, fetched, across):
    count = len(ranges)
    scales, sources, plain = refs[0], refs[1 : 1 + count], refs[1 + count : 1 + count + fetched]
    refs = refs[1 + count + fetched :]
    outs, fetch, held, sems = refs[:count], refs[count : count + fetched], refs[count + fetched : -1], refs[-1]
    jobs = []
    for source, to, out, (start, size) in zip(sources, held, outs, ranges):
        step = strip_rows((size, source.shape[1]))
        for first in range(0, size, step):
            copy = pltpu.make_async_copy(
                source.at[pl.ds(start + first, step)], to.at[pl.ds(first, step)], sems.at[len(jobs)]
            )
            jobs.append((copy, (out, to, scales, across, first // BLK, step // BLK, start // BLK)))
    direct = [pltpu.make_async_copy(a, to, sems.at[len(jobs) + i]) for i, (a, to) in enumerate(zip(plain, fetch))]
    for copy, _ in jobs[:DEPTH]:
        copy.start()
    for copy in direct:
        copy.start()
    for i, (copy, job) in enumerate(jobs):
        copy.wait()
        if i + DEPTH < len(jobs):
            jobs[i + DEPTH][0].start()
        dequantize_strips(*job)
    for copy in direct:
        copy.wait()


def prepared(scales, across, weights, fetch=()):
    codes = [item[0] for item in weights]
    ranges = tuple(item[1:] for item in weights)
    fetch = list(fetch)
    shapes = [(size, a.shape[1]) for a, (_, size) in zip(codes, ranges)]
    steps = sum(shape[0] // strip_rows(shape) for shape in shapes)
    return pl.pallas_call(
        functools.partial(prepare_body, ranges=ranges, fetched=len(fetch), across=across),
        in_specs=[SMEM] + [HBM] * (len(codes) + len(fetch)),
        out_specs=[VMEM] * (len(codes) + len(fetch)),
        out_shape=[pltpu.VMEM(shape, jnp.bfloat16) for shape in shapes] + [pltpu.VMEM(a.shape, a.dtype) for a in fetch],
        scratch_shapes=[pltpu.VMEM(shape, jnp.bfloat16) for shape in shapes]
        + [pltpu.SemaphoreType.DMA((steps + len(fetch),))],
        compiler_params=pltpu.CompilerParams(vmem_limit_bytes=2 * sum(math.prod(shape) for shape in shapes) + 2**20),
        name="prepare",
    )(scales, *(in_hbm(item) for item in codes + fetch))


def join_body(*refs):
    out = refs[-1]
    rows = refs[0].shape[0]
    for i, part in enumerate(refs[:-1]):
        out[i * rows : (i + 1) * rows, :] = part[...]


def joined(parts):
    rows, width = parts[0].shape
    return pl.pallas_call(
        join_body,
        in_specs=[VMEM] * len(parts),
        out_specs=VMEM,
        out_shape=jax.ShapeDtypeStruct((len(parts) * rows, width), parts[0].dtype),
        compiler_params=pltpu.CompilerParams(vmem_limit_bytes=SMALL_VMEM),
        name="join",
    )(*parts)


def expert_body(*refs, width, experts):
    parts = refs[: 2 * MID]
    gate_first, gate_rest, down, keep = refs[2 * MID : 2 * MID + 4]
    sends, x = refs[2 * MID + 4 : -1], refs[-1]
    expert = lax.axis_index("ctx") // 2
    some = parts[0].shape[0]
    half = keep.shape[0]
    for i, part in enumerate(parts):
        x[i * some : (i + 1) * some, :] = part[:, 0:width]
    tail = jnp.concatenate([part[:, width:] for part in parts], axis=0).astype(jnp.float32)
    lane = lax.broadcasted_iota(jnp.int32, tail.shape, 1)
    chosen = (lane == expert) | (lane == expert + experts)
    weight = jnp.sum(jnp.where(chosen, tail, 0.0), axis=1, keepdims=True)
    hidden = down.shape[0]
    first = gate_first.shape[0]
    act = jnp.dot(x[:, :first], gate_first[...], preferred_element_type=jnp.float32)
    act += jnp.dot(x[:, first:], gate_rest[...], preferred_element_type=jnp.float32)
    gate, up = act[:, :hidden], act[:, hidden:]
    active = (gate / (1.0 + jnp.exp(-gate)) * up).astype(jnp.bfloat16)
    out = jnp.dot(active, down[...], preferred_element_type=jnp.float32) * weight
    keep[...] = out[0:half]
    for i, send in enumerate(sends):
        count = send.shape[0]
        send[...] = out[half + i * count : half + (i + 1) * count].astype(jnp.bfloat16)


VMEM = pl.BlockSpec(memory_space=pltpu.VMEM)
SMEM = pl.BlockSpec(memory_space=pltpu.SMEM)
HBM = pl.BlockSpec(memory_space=pltpu.HBM)
ANY = pl.BlockSpec(memory_space=pl.ANY)


def add_body(keep, got, out, *, first):
    out[...] = (keep[first : first + out.shape[0], :] + got[...].astype(jnp.float32)).astype(out.dtype)


def added(keep, got, first):
    return pl.pallas_call(
        functools.partial(add_body, first=first),
        in_specs=[VMEM] * 2,
        out_specs=VMEM,
        out_shape=jax.ShapeDtypeStruct(got.shape, got.dtype),
        compiler_params=pltpu.CompilerParams(vmem_limit_bytes=keep.size * 4 + got.size * 8 + 2**20),
        name="add",
    )(keep, got)


def scatter_sum(keep, sends, mid, high):
    width = keep.shape[1]
    step = sends[0].shape[0]
    order = (*range(1, len(mid)), 0)
    came = {i: swapped(sends[i], 1) for i in order}
    total = keep[:step] + came[0].astype(jnp.float32)
    got = [swapped(added(keep, came[i], i * step), mid[i]) for i in order[:-1]]
    for item in got:
        total = total + item.astype(jnp.float32)
    parts = total.reshape(len(high), -1, width)
    total = parts[0]
    got = [swapped(parts[i].astype(jnp.bfloat16), high[i]) for i in range(1, len(high))]
    for item in got:
        total = total + item.astype(jnp.float32)
    return total


def local(
    queries,
    own_key,
    own_value,
    cache_keys,
    cache_values,
    prefix_of_row,
    context_len,
    hidden_in,
    w_out,
    norm_gain,
    expert_ids,
    route_weights,
    gate_up_codes,
    gate_up_scales,
    down_codes,
    down_scales,
):
    shards = lax.axis_size("ctx")
    device = lax.axis_index("ctx")
    rows = queries.shape[0]
    width = hidden_in.shape[1]
    key_groups = own_key.shape[1] // HD
    head_count = queries.shape[1] // HD
    per_group = head_count // key_groups
    prefixes, ctx_local, _ = cache_keys.shape
    kv_rows = prefixes * ctx_local
    feature = w_out.shape[0]
    low, mid, high = stage_offsets(shards)
    tables = (prefix_of_row, context_len, gate_up_scales.transpose(2, 0, 1), down_scales.transpose(1, 0, 2))

    inputs = (queries, own_key, own_value, cache_keys, cache_values)
    message = jax.ShapeDtypeStruct((kv_rows + MID * rows + 2 * rows, 2 * HD), jnp.bfloat16)
    near = jax.ShapeDtypeStruct((kv_rows + 2 * rows, 2 * HD), jnp.bfloat16)
    count = MID + len(high) - 1
    steps = len(inputs) + len(tables)
    packed = pl.pallas_call(
        functools.partial(pack_body, feature=feature, per_group=per_group, count=count, tables=len(tables)),
        in_specs=[HBM] * steps,
        out_specs=[VMEM] * (count + len(tables)),
        out_shape=[near] * MID + [message] * (len(high) - 1) + [jax.ShapeDtypeStruct(a.shape, a.dtype) for a in tables],
        scratch_shapes=[pltpu.VMEM(a.shape, a.dtype) for a in inputs] + [pltpu.SemaphoreType.DMA((steps,))],
        compiler_params=pltpu.CompilerParams(vmem_limit_bytes=SMALL_VMEM),
        name="pack",
    )(*(in_hbm(item) for item in inputs + tables))
    prefix_of, lengths, gate_scales, low_scales = packed[count:]
    got = [swapped(item, offset) for item, offset in zip(packed[MID:count], high[1:])]
    mine_near = [packed[0]] + [swapped(packed[i], mid[i]) for i in range(1, MID)]
    piece = jax.ShapeDtypeStruct((len(high) - 1, kv_rows + 2 * rows, 2 * HD), jnp.bfloat16)
    messages = pl.pallas_call(
        functools.partial(repack_body, kv_rows=kv_rows, rows=rows),
        in_specs=[VMEM] * len(got),
        out_specs=[VMEM] * MID,
        out_shape=[piece] * MID,
        compiler_params=pltpu.CompilerParams(vmem_limit_bytes=2 * SMALL_VMEM),
        name="repack",
    )(*got)
    mine = [messages[0]] + [swapped(messages[i], mid[i]) for i in range(1, MID)]
    other_near = [swapped(item, low[1]) for item in mine_near]
    other = [swapped(item, low[1]) for item in mine]

    if feature < HD:
        w_full = lax.dynamic_update_slice(
            jnp.zeros((HD, w_out.shape[1]), w_out.dtype), w_out, ((device * feature) % HD, 0)
        )
    else:
        w_full = w_out
    codes = gate_up_codes[0]
    first = codes.shape[0] // 2
    gate_first, w_full = prepared(gate_scales, True, [(codes, 0, first)], [w_full])
    (down,) = prepared(low_scales, False, [(down_codes[0], 0, down_codes.shape[1])])
    (gate_rest,) = prepared(gate_scales, True, [(codes, first, codes.shape[0] - first)])
    half = shards * rows // 2
    attend_vmem = 8 * 2**20 + 2 * MID * (piece.size + near.size) * 2 + w_full.size * 2 + half * width * 10
    keep, *sends = pl.pallas_call(
        functools.partial(attend_body, ctx_local=ctx_local, kv_rows=kv_rows, rows=rows),
        in_specs=[SMEM] * 2 + [VMEM] * (4 * MID + 1),
        out_specs=[VMEM] * (1 + MID),
        out_shape=[
            jax.ShapeDtypeStruct((half, width), jnp.float32),
            *[jax.ShapeDtypeStruct((half // MID, width), jnp.bfloat16)] * MID,
        ],
        scratch_shapes=[
            pltpu.VMEM((LOW * MID, len(high) * rows, HD), jnp.float32),
        ],
        compiler_params=pltpu.CompilerParams(vmem_limit_bytes=attend_vmem),
        name="attend",
    )(prefix_of, lengths, *mine_near, *mine, *other_near, *other, w_full)

    projected = scatter_sum(keep, sends, mid, high)
    mixed = hidden_in.astype(jnp.float32) + projected
    attention_out = mixed.astype(jnp.bfloat16)
    mean_square = jnp.mean(mixed * mixed, axis=-1, keepdims=True)
    normed = (mixed * lax.rsqrt(mean_square + EPSILON) * norm_gain).astype(jnp.bfloat16)

    experts_all = shards // 2
    hit = expert_ids[:, :, None] == jnp.arange(experts_all, dtype=jnp.int32)[None, None, :]
    combine = jnp.sum(jnp.where(hit, route_weights[:, :, None], 0.0), axis=1)
    coarse = lax.reduce_precision(combine, 8, 7)
    fine = combine - coarse
    extra = -(2 * experts_all) % HD
    tail = jnp.concatenate([coarse, fine, jnp.zeros((rows, extra), jnp.float32)], axis=1)
    held = jnp.concatenate([normed, tail.astype(jnp.bfloat16)], axis=1)
    held = joined([held] + [swapped(held, o) for o in high[1:]])
    mine = [held] + [swapped(held, o) for o in mid[1:]]
    other = [swapped(item, low[1]) for item in mine]
    expert_vmem = 4 * 2**20 + 2 * half * width * 15
    keep, *sends = pl.pallas_call(
        functools.partial(expert_body, width=width, experts=experts_all),
        in_specs=[VMEM] * (2 * MID + 3),
        out_specs=[VMEM] * (1 + MID),
        out_shape=[
            jax.ShapeDtypeStruct((half, width), jnp.float32),
            *[jax.ShapeDtypeStruct((half // MID, width), jnp.bfloat16)] * MID,
        ],
        scratch_shapes=[
            pltpu.VMEM((2 * half, width), jnp.bfloat16),
        ],
        compiler_params=pltpu.CompilerParams(vmem_limit_bytes=expert_vmem),
        name="expert",
    )(*mine, *other, gate_first, gate_rest, down)
    expert_sum = scatter_sum(keep, sends, mid, high)
    layer_out = (mixed + expert_sum).astype(jnp.bfloat16)
    return (attention_out, layer_out)


def solution(mesh):
    return jax.shard_map(
        local,
        mesh=mesh,
        in_specs=(
            P(("replica", "ctx"), None),
            P(("replica", "ctx"), None),
            P(("replica", "ctx"), None),
            P("replica", "ctx", None),
            P("replica", "ctx", None),
            P("replica"),
            P("replica"),
            P(("replica", "ctx"), None),
            P("ctx", None),
            P(),
            P(("replica", "ctx"), None),
            P(("replica", "ctx"), None),
            P("ctx", None, None),
            P("ctx", None, None),
            P("ctx", None, None),
            P("ctx", None, None),
        ),
        out_specs=(P(("replica", "ctx"), None), P(("replica", "ctx"), None)),
        check_vma=False,
    )
```
